32 devices in a mesh: dp: 32 (over z, y, x, core).
Axes of the slice: x: 2, y: 2, z: 4, core: 2. Of those that a mesh axis runs over, the one named last changes fastest.
Arguments:
- features: bfloat16 [256, 128, 1024], P('dp'), may hold values from -16 to 16
- ln_gain: float32 [1024], replicated, may hold values from 0.5 to 1.5
- w_query: bfloat16 [1024, 1024], replicated, may hold values from -0.1875 to 0.1875
- w_key: bfloat16 [1024, 1024], replicated, may hold values from -0.1875 to 0.1875
- w_value: bfloat16 [1024, 1024], replicated, may hold values from -0.1875 to 0.1875
- w_out: bfloat16 [1024, 1024], replicated, may hold values from -0.1875 to 0.1875
- text_raw: bfloat16 [256, 1024], P('dp'), may hold values from -0.35 to 0.35
Outputs:
- loss: float32 [], replicated
- text_grad: float32 [256, 1024], P('dp')
- w_out_grad: bfloat16 [1024, 1024], replicated
The draws below stay inside these ranges and needn't reach their ends.
All inputs are finite; a program needn't handle non-finite values.
Results may differ from the reference program's by a relative error of at most 0.009.
Values may be sent and summed in bfloat16 or wider, within the bound.
A program may use at most 128 MiB of HBM per device.

```python
import jax
import jax.numpy as jnp
from jax import lax

D = 1024
HEADS = 16
PATCHES = 127
BATCH = 256


def unit_noise(rng_key, shape):
    return jax.random.truncated_normal(rng_key, -4.0, 4.0, shape, jnp.float32)


def paired_rows(key):
    folded = jax.random.fold_in(key, 1031)
    streams = jax.random.split(folded, 7)
    common = unit_noise(streams[0], (1, D))
    shared = unit_noise(streams[1], (BATCH, D))
    image_noise = unit_noise(streams[2], (BATCH, D))
    text_noise = unit_noise(streams[3], (BATCH, D))
    order = jax.random.permutation(streams[6], BATCH).astype(jnp.int32)
    partner = jnp.zeros((BATCH,), jnp.int32).at[order].set(jnp.roll(order, -1))
    mate_rows = shared[partner]
    ramp = jnp.arange(BATCH, dtype=jnp.float32)[:, None] / BATCH
    image_scale = jax.random.uniform(streams[4], (BATCH, 1), jnp.float32, 0.3, 0.7)
    text_scale = jax.random.uniform(streams[5], (BATCH, 1), jnp.float32, 0.0, 0.9)
    noise_scale = 0.4 + 1.6 * ramp
    class_rows = image_scale * common + shared + 0.7 * mate_rows + noise_scale * image_noise
    text_rows = 0.03125 * (text_scale * common + shared + 0.8 * text_noise)
    return (class_rows, text_rows)


def draw_features(key, part):
    class_rows, text_rows = paired_rows(key)
    patch_rows = unit_noise(jax.random.fold_in(key, 2063), (BATCH, PATCHES, D))
    return jnp.concatenate([class_rows[:, None, :], patch_rows], axis=1).astype(jnp.bfloat16)


def draw_text_raw(key, part):
    class_rows, text_rows = paired_rows(key)
    return text_rows.astype(jnp.bfloat16)


def normal_values(key, extent, scale, bound, kind=jnp.bfloat16):
    entries = scale * jax.random.normal(key, extent, jnp.float32)
    return jnp.clip(entries, min=-bound, max=bound).astype(kind)


def setup_inputs(seed: int = 0) -> dict:
    key_of = jax.random.split(jax.random.key(seed), 8)
    return {
        "features": draw_features(jax.random.fold_in(key_of[7], 71), 0),
        "ln_gain": jnp.clip(1.0 + 0.1 * jax.random.normal(key_of[1], (D,), jnp.float32), 0.5, 1.5),
        "w_query": normal_values(key_of[2], (D, D), D ** -0.5, 0.1875),
        "w_key": normal_values(key_of[3], (D, D), D ** -0.5, 0.1875),
        "w_value": normal_values(key_of[4], (D, D), D ** -0.5, 0.1875),
        "w_out": normal_values(key_of[5], (D, D), D ** -0.5, 0.1875),
        "text_raw": draw_text_raw(jax.random.fold_in(key_of[7], 71), 0),
    }


inv_temp = 1.0 / 0.07
attn_temp = 8.0
epsilon = 1e-06

def layer_norm(inputs, gain):
    center = inputs - lax.optimization_barrier(jnp.mean(inputs, axis=-1, keepdims=True))
    spread = lax.optimization_barrier(jnp.mean(center * center, axis=-1, keepdims=True))
    return center * lax.rsqrt(spread + epsilon) * gain

def unit_heads(proj, heads):
    shaped = proj.reshape(proj.shape[0], proj.shape[1], heads, -1)
    return (shaped * lax.rsqrt(lax.optimization_barrier(jnp.sum(shaped * shaped, axis=-1, keepdims=True)) + epsilon)).astype(jnp.bfloat16)

def embed(feats, ln_gain, w_query, w_key, w_value, w_out):
    images, tokens, width = feats.shape
    inputs = feats.astype(jnp.float32)
    normed = layer_norm(inputs, ln_gain).astype(jnp.bfloat16).reshape(images * tokens, width)
    query = unit_heads(jnp.dot(normed, w_query, preferred_element_type=jnp.float32).reshape(images, tokens, width), HEADS)
    key_heads = unit_heads(jnp.dot(normed, w_key, preferred_element_type=jnp.float32).reshape(images, tokens, width), HEADS)
    value_heads = jnp.dot(normed, w_value, preferred_element_type=jnp.float32).reshape(images, tokens, HEADS, -1).astype(jnp.bfloat16)
    scores = attn_temp * jnp.einsum('bqhd,bkhd->bhqk', query.astype(jnp.float32), key_heads.astype(jnp.float32))
    expo = jnp.exp(scores)
    weights = (expo / lax.optimization_barrier(jnp.sum(expo, axis=-1, keepdims=True))).astype(jnp.bfloat16).astype(jnp.float32)
    pooled = weights[:, :, 0, :] + lax.optimization_barrier(jnp.mean(weights[:, :, 1:, :], axis=2))
    abar = jnp.einsum('bhk,bkhd->bhd', pooled, value_heads.astype(jnp.float32), precision=lax.Precision.HIGHEST)
    abar = abar.reshape(images, width).astype(jnp.bfloat16)
    xbar = inputs[:, 0, :] + lax.optimization_barrier(jnp.mean(inputs[:, 1:, :], axis=1))
    emb = xbar + jnp.dot(abar, w_out, preferred_element_type=jnp.float32)
    return (emb, abar)

def reference(features, ln_gain, w_query, w_key, w_value, w_out, text_raw):

    def one_image(single):
        return embed(single[None], ln_gain, w_query, w_key, w_value, w_out)
    emb, abar = lax.map(one_image, features)
    emb = emb.reshape(BATCH, D)
    abar = abar.reshape(BATCH, D)
    emb_norm = jnp.sqrt(lax.optimization_barrier(jnp.sum(emb * emb, axis=1, keepdims=True)) + epsilon)
    img_f = emb / emb_norm
    img_u = img_f.astype(jnp.bfloat16)
    text32 = text_raw.astype(jnp.float32)
    txt_norm = jnp.sqrt(lax.optimization_barrier(jnp.sum(text32 * text32, axis=1, keepdims=True)) + epsilon)
    txt_f = text32 / txt_norm
    txt_u = txt_f.astype(jnp.bfloat16)
    logits = inv_temp * jnp.dot(img_u, txt_u.T, preferred_element_type=jnp.float32)
    exp_logits = jnp.exp(logits)
    rowsum = lax.optimization_barrier(jnp.sum(exp_logits, axis=1))
    colsum = lax.optimization_barrier(jnp.sum(exp_logits, axis=0))
    diag_logit = jnp.diagonal(logits)
    loss = (jnp.sum(jnp.log(rowsum) - diag_logit) + jnp.sum(jnp.log(colsum) - diag_logit)) / (2.0 * BATCH)
    delta = 0.5 * (exp_logits / rowsum[:, None] + exp_logits / colsum[None, :]) - jnp.eye(BATCH, dtype=jnp.float32)
    delta = delta.astype(jnp.bfloat16)
    grad_img = inv_temp * jnp.dot(delta, txt_u, preferred_element_type=jnp.float32)
    grad_txt = inv_temp * jnp.dot(delta.T, img_u, preferred_element_type=jnp.float32)
    text_grad = (grad_txt - txt_f * lax.optimization_barrier(jnp.sum(txt_f * grad_txt, axis=1, keepdims=True))) / txt_norm
    emb_grad = (grad_img - img_f * lax.optimization_barrier(jnp.sum(img_f * grad_img, axis=1, keepdims=True))) / emb_norm
    w_out_grad = jnp.dot(abar.astype(jnp.float32).T, emb_grad, precision=lax.Precision.HIGHEST).astype(jnp.bfloat16)
    return (loss, text_grad, w_out_grad)
```

```python
import functools

import jax
import jax.numpy as jnp
from jax import lax
from jax.experimental import pallas as pl
from jax.experimental.pallas import tpu as pltpu
from jax.sharding import PartitionSpec as P

HEADS = 16
GROUP = 4
BLOCKS = 2

inv_temp = 1.0 / 0.07
attn_temp = 8.0
epsilon = 1e-06
log2e = 1.4426950408889634

F32 = jnp.float32
BF16 = jnp.bfloat16
NT = (((1,), (1,)), ((), ()))
TN = (((0,), (0,)), ((), ()))


MESH = pl.DeviceIdType.MESH


def target(n, i):
    return lax.rem(lax.axis_index("dp") + 2 * i, n)


def mate():
    me = lax.axis_index("dp")
    return me + 1 - 2 * lax.rem(me, 2)


def greet(n):
    barrier = pltpu.get_barrier_semaphore()

    def hello(i, _):
        pl.semaphore_signal(barrier, inc=1, device_id=(target(n, i),), device_id_type=MESH)
        return 0

    pl.semaphore_signal(barrier, inc=1, device_id=(mate(),), device_id_type=MESH)
    lax.fori_loop(1, n // 2, hello, 0)


class Share:
    def __init__(self, n, src, out, sems, own_sem):
        self.n, self.src, self.out, self.sems = n, src, out, sems
        self.half = n // 2
        self.own = pltpu.make_async_copy(src, out.at[lax.axis_index("dp")], own_sem)

    def direct(self, i):
        return pltpu.make_async_remote_copy(
            src_ref=self.src,
            dst_ref=self.out.at[lax.axis_index("dp")],
            send_sem=self.sems.at[0, i],
            recv_sem=self.sems.at[1, i],
            device_id=(target(self.n, i),),
            device_id_type=MESH,
        )

    def relay(self, i):
        slot = lax.rem(lax.axis_index("dp") - 2 * i + self.n, self.n)
        return pltpu.make_async_remote_copy(
            src_ref=self.out.at[slot],
            dst_ref=self.out.at[slot],
            send_sem=self.sems.at[2, i],
            recv_sem=self.sems.at[3, i],
            device_id=(mate(),),
            device_id_type=MESH,
        )

    def each(self, low, act):
        def step(i, _):
            act(i)
            return 0

        lax.fori_loop(low, self.half, step, 0)

    def start(self):
        self.own.start()
        self.each(1, lambda i: self.direct(i).start())

    def forward(self):
        self.own.wait()
        self.relay(0).start()

        def pass_on(i):
            self.direct(i).wait_recv()
            self.relay(i).start()

        self.each(1, pass_on)

    def finish(self):
        self.each(1, lambda i: self.direct(i).wait_send())

        def drain(i):
            self.relay(i).wait_send()
            self.relay(i).wait_recv()

        self.each(0, drain)


class LineShare:
    def __init__(self, n, lines, src, out, sems, own_sem):
        self.n, self.lines, self.src, self.out, self.sems = n, lines, src, out, sems
        self.plane = n // lines
        self.peers = self.plane // 2
        self.me = lax.axis_index("dp")
        self.spot = lax.rem(self.me, self.plane)
        self.own = pltpu.make_async_copy(src, out.at[self.me], own_sem)

    def block(self, j, k):
        owner = self.me - self.spot + lax.rem(self.spot - 2 * k + self.plane, self.plane)
        return self.out.at[lax.rem(owner - self.plane * j + self.n, self.n)]

    def copy(self, kind, j, k, src, dst, device):
        return pltpu.make_async_remote_copy(
            src_ref=src,
            dst_ref=dst,
            send_sem=self.sems.at[2 * kind, j, k],
            recv_sem=self.sems.at[2 * kind + 1, j, k],
            device_id=(device,),
            device_id_type=MESH,
        )

    def along(self, j):
        device = lax.rem(self.me + self.plane * j, self.n)
        return self.copy(0, j, 0, self.src, self.out.at[self.me], device)

    def across(self, j, k):
        device = self.me - self.spot + lax.rem(self.spot + 2 * k, self.plane)
        here = self.block(j, 0)
        return self.copy(1, j, k, self.src if j == 0 else here, here, device)

    def relay(self, j, k):
        here = self.block(j, k)
        return self.copy(2, j, k, here, here, mate())

    def each(self, low, act):
        def step(k, _):
            act(k)
            return 0

        lax.fori_loop(low, self.peers, step, 0)

    def run(self):
        self.own.start()
        for j in range(1, self.lines):
            self.along(j).start()
        self.each(1, lambda k: self.across(0, k).start())
        self.own.wait()
        self.relay(0, 0).start()
        for j in range(1, self.lines):
            self.along(j).wait_recv()
            self.each(1, lambda k: self.across(j, k).start())
            self.relay(j, 0).start()

        for j in range(self.lines):

            def pass_on(k):
                self.across(j, k).wait_recv()
                self.relay(j, k).start()

            self.each(1, pass_on)
        for j in range(1, self.lines):
            self.along(j).wait_send()
        for j in range(self.lines):
            self.each(1, lambda k: self.across(j, k).wait_send())

            def drain(k):
                self.relay(j, k).wait_send()
                self.relay(j, k).wait_recv()

            self.each(0, drain)


def line_count(n):
    return 4 if n % 8 == 0 else 1


def embed_kernel(
    n,
    x_hbm,
    gain_ref,
    wq_hbm,
    wk_hbm,
    wv_hbm,
    wo_hbm,
    text_ref,
    all_img,
    all_txt,
    msg_ref,
    txt_ref,
    xs,
    wqks,
    wvs,
    wos,
    normed,
    qkn0,
    qkn1,
    pooled,
    zhi,
    zlo,
    xbar,
    x_sem,
    q_sem,
    k_sem,
    v_sem,
    o_sem,
    img_sems,
    txt_sems,
    own_sem,
):
    images, tokens, width = xs.shape
    groups = wqks.shape[0]
    cols = width // groups
    head = width // HEADS

    def x_copy(i):
        return pltpu.make_async_copy(x_hbm.at[i], xs.at[i], x_sem.at[i])

    def q_copy(g):
        return pltpu.make_async_copy(wq_hbm.at[:, pl.ds(g * cols, cols)], wqks.at[g, :, pl.ds(0, cols)], q_sem.at[g])

    def k_copy(g):
        return pltpu.make_async_copy(wk_hbm.at[:, pl.ds(g * cols, cols)], wqks.at[g, :, pl.ds(cols, cols)], k_sem.at[g])

    v_copy = pltpu.make_async_copy(wv_hbm, wvs, v_sem)
    o_copy = pltpu.make_async_copy(wo_hbm, wos, o_sem)
    for i in range(images):
        x_copy(i).start()
    for g in range(groups):
        q_copy(g).start()
        k_copy(g).start()
    v_copy.start()
    o_copy.start()

    greet(n)
    text32 = text_ref[...].astype(F32)
    txt_norm = jnp.sqrt(jnp.sum(text32 * text32, axis=1, keepdims=True) + epsilon)
    txt_ref[...] = (text32 / txt_norm).astype(BF16)
    txt_share = Share(n, txt_ref, all_txt, txt_sems, own_sem.at[0])
    img_share = LineShare(n, line_count(n), msg_ref, all_img, img_sems, own_sem.at[1])

    gain = gain_ref[...]
    block = 32
    blocks = BLOCKS

    def norm_image(i, _):
        x_copy(i).wait()

        def norm_block(b, acc):
            x = xs[i, pl.ds(b * block, block), :].astype(F32)
            center = x - jnp.mean(x, axis=-1, keepdims=True)
            spread = jnp.mean(center * center, axis=-1, keepdims=True)
            out = center * lax.rsqrt(spread + epsilon) * gain
            rows = pl.ds(pl.multiple_of(i * tokens + b * block, block), block)
            normed[rows, :] = out.astype(BF16)
            return acc + jnp.sum(x, axis=0, keepdims=True)

        total = lax.fori_loop(0, tokens // block, norm_block, jnp.zeros((1, width), F32), unroll=4)
        first = xs[i, pl.ds(0, 1), :].astype(F32)
        xbar[pl.ds(i, 1), :] = first + (total - first) / (tokens - 1)
        return 0

    lax.fori_loop(0, images, norm_image, 0)

    seg_row = lax.broadcasted_iota(jnp.int32, (cols, cols), 0) // head
    seg_col = lax.broadcasted_iota(jnp.int32, (cols, cols), 1) // head
    seg = jnp.where(seg_row == seg_col, 1.0, 0.0).astype(BF16)
    lanes = 128
    per = lanes // head
    lane_head = lax.broadcasted_iota(jnp.int32, (tokens, lanes), 1) // head
    coef = jnp.where(
        lax.broadcasted_iota(jnp.int32, (tokens, 1), 0) == 0, 1.0, 1.0 / (tokens - 1)
    ).astype(F32)

    def unit(proj):
        sq = jnp.dot((proj * proj).astype(BF16), seg, preferred_element_type=F32)
        return (proj * lax.rsqrt(sq + epsilon)).astype(BF16)

    def project(g, b):
        rows = pl.ds(b * (images * tokens // blocks), images * tokens // blocks)
        proj = jnp.dot(normed[rows, :], wqks[g], preferred_element_type=F32)
        qkn = qkns[g % 2]
        qkn[rows, 0:cols] = unit(proj[:, 0:cols])
        qkn[rows, cols : 2 * cols] = unit(proj[:, cols : 2 * cols])

    def attend(g, i):
        rows = pl.ds(i * tokens, tokens)
        qkn = qkns[g % 2]
        for pair in range(cols // lanes):
            lo = pair * lanes
            qi = qkn[rows, lo : lo + lanes]
            ki = qkn[rows, cols + lo : cols + lo + lanes]
            km = jnp.concatenate(
                [jnp.where(lane_head == h, ki, jnp.zeros_like(ki)) for h in range(per)],
                axis=0,
            )
            s = lax.dot_general(qi, km, NT, preferred_element_type=F32)
            e = jnp.exp2(s * (attn_temp * log2e))
            for h in range(per):
                eh = e[:, h * tokens : (h + 1) * tokens]
                scale = coef / jnp.sum(eh, axis=-1, keepdims=True)
                ph = jnp.sum(eh * scale, axis=0, keepdims=True)
                at = g * (cols // head) + pair * per + h
                pooled[i, at : at + 1, :] = ph

    qkns = (qkn0, qkn1)
    for g in range(groups + 1):
        if g < groups:
            q_copy(g).wait()
            k_copy(g).wait()
        if g == 1:
            pl.semaphore_wait(pltpu.get_barrier_semaphore(), n // 2)
            txt_share.start()
        for b in range(blocks):
            if g > 0:
                for i in range(b * images // blocks, (b + 1) * images // blocks):
                    attend(g - 1, i)
            if g < groups:
                project(g, b)

    txt_share.forward()

    for i in range(images):
        p = pooled[i]
        hi = p.astype(BF16)
        lo = (p - hi.astype(F32)).astype(BF16)
        z2 = jnp.dot(
            jnp.concatenate([hi, lo], axis=0),
            normed[i * tokens : (i + 1) * tokens, :],
            preferred_element_type=F32,
        )
        z = z2[:HEADS] + z2[HEADS:]
        hi = z.astype(BF16)
        zhi[i * HEADS : (i + 1) * HEADS, :] = hi
        zlo[i * HEADS : (i + 1) * HEADS, :] = (z - hi.astype(F32)).astype(BF16)

    v_copy.wait()
    o_copy.wait()
    full = jnp.dot(zhi[...], wvs[...], preferred_element_type=F32) + jnp.dot(
        zlo[...], wvs[...], preferred_element_type=F32
    )
    own_head = lax.broadcasted_iota(jnp.int32, (HEADS, width), 0) == (
        lax.broadcasted_iota(jnp.int32, (HEADS, width), 1) // head
    )
    picked = [
        jnp.sum(
            jnp.where(own_head, full[i * HEADS : (i + 1) * HEADS, :], 0.0), axis=0, keepdims=True
        )
        for i in range(images)
    ]
    abar = jnp.concatenate(picked, axis=0).astype(BF16)
    emb = xbar[...] + jnp.dot(abar, wos[...], preferred_element_type=F32)
    emb_norm = jnp.sqrt(jnp.sum(emb * emb, axis=1, keepdims=True) + epsilon)
    n0 = emb_norm.astype(BF16).astype(F32)
    n1 = (emb_norm - n0).astype(BF16).astype(F32)
    n2 = emb_norm - n0 - n1
    lane = lax.broadcasted_iota(jnp.int32, (images, 128), 1)
    tail = jnp.where(lane == 0, n0, jnp.where(lane == 1, n1, jnp.where(lane == 2, n2, 0.0)))
    msg_ref[:, 0:width] = (emb / emb_norm).astype(BF16)
    msg_ref[:, width : 2 * width] = abar
    msg_ref[:, 2 * width :] = tail.astype(BF16)
    img_share.run()
    txt_share.finish()


def embed(features, ln_gain, w_query, w_key, w_value, w_out, text_raw, n):
    images, tokens, width = features.shape
    groups = HEADS // GROUP
    cols = width // groups
    hbm = pl.BlockSpec(memory_space=pl.ANY)
    vmem = pl.BlockSpec(memory_space=pltpu.VMEM)
    return pl.pallas_call(
        functools.partial(embed_kernel, n),
        out_shape=(
            jax.ShapeDtypeStruct((n, images, 2 * width + 128), BF16),
            jax.ShapeDtypeStruct((n, images, width), BF16),
        ),
        in_specs=[hbm, vmem, hbm, hbm, hbm, hbm, vmem],
        out_specs=(vmem, vmem),
        scratch_shapes=[
            pltpu.VMEM((images, 2 * width + 128), BF16),
            pltpu.VMEM((images, width), BF16),
            pltpu.VMEM((images, tokens, width), BF16),
            pltpu.VMEM((groups, width, 2 * cols), BF16),
            pltpu.VMEM((width, width), BF16),
            pltpu.VMEM((width, width), BF16),
            pltpu.VMEM((images * tokens, width), BF16),
            pltpu.VMEM((images * tokens, 2 * cols), BF16),
            pltpu.VMEM((images * tokens, 2 * cols), BF16),
            pltpu.VMEM((images, HEADS, tokens), F32),
            pltpu.VMEM((images * HEADS, width), BF16),
            pltpu.VMEM((images * HEADS, width), BF16),
            pltpu.VMEM((images, width), F32),
            pltpu.SemaphoreType.DMA((images,)),
            pltpu.SemaphoreType.DMA((groups,)),
            pltpu.SemaphoreType.DMA((groups,)),
            pltpu.SemaphoreType.DMA,
            pltpu.SemaphoreType.DMA,
            pltpu.SemaphoreType.DMA((6, line_count(n), n // line_count(n) // 2)),
            pltpu.SemaphoreType.DMA((4, n // 2)),
            pltpu.SemaphoreType.DMA((2,)),
        ],
        compiler_params=pltpu.CompilerParams(collective_id=0, has_side_effects=True),
        name="embed",
    )(features, ln_gain.reshape(1, width), w_query, w_key, w_value, w_out, text_raw)


def loss_kernel(all_ref, txt_all_ref, text_ref, me_ref, loss_ref, text_grad_ref, w_grad_ref):
    total = all_ref.shape[0]
    images, width = text_ref.shape
    img = all_ref[:, 0:width]
    txt = txt_all_ref[...]
    logits = inv_temp * lax.dot_general(img, txt, NT, preferred_element_type=F32)
    e = jnp.exp(logits)
    flipped = jnp.exp(inv_temp * lax.dot_general(txt, img, NT, preferred_element_type=F32))
    rowsum = jnp.sum(e, axis=1, keepdims=True)
    colsum = jnp.sum(e, axis=0, keepdims=True)
    rowsum_flat = jnp.sum(flipped, axis=0, keepdims=True)
    eye = lax.broadcasted_iota(jnp.int32, (total, total), 0) == lax.broadcasted_iota(
        jnp.int32, (total, total), 1
    )
    diag = jnp.sum(jnp.where(eye, logits, 0.0))
    loss = (jnp.sum(jnp.log(rowsum_flat)) + jnp.sum(jnp.log(colsum)) - 2.0 * diag) / (2.0 * total)
    loss_ref[0, 0] = loss

    delta = 0.5 * (e / rowsum + e / colsum) - jnp.where(eye, 1.0, 0.0)
    grad_img = inv_temp * jnp.dot(delta.astype(BF16), txt, preferred_element_type=F32)
    norms = all_ref[:, 2 * width :].astype(F32)
    emb_norm = jnp.sum(norms, axis=1, keepdims=True)
    img32 = img.astype(F32)
    emb_grad = (grad_img - img32 * jnp.sum(img32 * grad_img, axis=1, keepdims=True)) / emb_norm
    hi = emb_grad.astype(BF16)
    lo = (emb_grad - hi.astype(F32)).astype(BF16)
    abar = all_ref[:, width : 2 * width]
    w_grad = lax.dot_general(abar, hi, TN, preferred_element_type=F32) + lax.dot_general(
        abar, lo, TN, preferred_element_type=F32
    )
    w_grad_ref[...] = w_grad.astype(BF16)

    text32 = text_ref[...].astype(F32)
    txt_norm = jnp.sqrt(jnp.sum(text32 * text32, axis=1, keepdims=True) + epsilon)
    txt_f = text32 / txt_norm
    own = inv_temp * lax.dot_general(
        txt_f.astype(BF16), img, NT, preferred_element_type=F32
    )
    own_e = jnp.exp(own)
    own_sum = jnp.sum(own_e, axis=1, keepdims=True)
    col = lax.broadcasted_iota(jnp.int32, (images, total), 1)
    row = lax.broadcasted_iota(jnp.int32, (images, total), 0) + me_ref[0] * images
    own_delta = 0.5 * (own_e / rowsum_flat + own_e / own_sum) - jnp.where(col == row, 1.0, 0.0)
    grad_txt = inv_temp * jnp.dot(own_delta.astype(BF16), img, preferred_element_type=F32)
    text_grad_ref[...] = (
        grad_txt - txt_f * jnp.sum(txt_f * grad_txt, axis=1, keepdims=True)
    ) / txt_norm


def finish(all_img, all_txt, text_raw):
    images, width = text_raw.shape
    vmem = pl.BlockSpec(memory_space=pltpu.VMEM)
    smem = pl.BlockSpec(memory_space=pltpu.SMEM)
    me = lax.axis_index("dp").astype(jnp.int32).reshape(1)
    loss, text_grad, w_grad = pl.pallas_call(
        loss_kernel,
        out_shape=(
            jax.ShapeDtypeStruct((1, 1), F32),
            jax.ShapeDtypeStruct((images, width), F32),
            jax.ShapeDtypeStruct((width, width), BF16),
        ),
        in_specs=[vmem, vmem, vmem, smem],
        out_specs=(smem, vmem, vmem),
        name="finish",
    )(all_img, all_txt, text_raw, me)
    return loss.reshape(()), text_grad, w_grad


def solution(mesh):
    n = mesh.shape["dp"]

    def local(features, ln_gain, w_query, w_key, w_value, w_out, text_raw):
        all_img, all_txt = embed(
            features, ln_gain, w_query, w_key, w_value, w_out, text_raw, n
        )
        pairs = n * text_raw.shape[0]
        return finish(all_img.reshape(pairs, -1), all_txt.reshape(pairs, -1), text_raw)

    placed = (P("dp", None, None), P(), P(), P(), P(), P(), P("dp", None))
    return jax.shard_map(
        local, mesh=mesh, in_specs=placed, out_specs=(P(), P("dp", None), P()), check_vma=False
    )
```

```python
import functools

import jax
import jax.numpy as jnp
from jax import lax
from jax.experimental import pallas as pl
from jax.experimental.pallas import tpu as pltpu
from jax.sharding import PartitionSpec as P

HEADS = 16
GROUP = 4
BLOCKS = 2
SLOTS = 8

inv_temp = 1.0 / 0.07
attn_temp = 8.0
epsilon = 1e-06
log2e = 1.4426950408889634

F32 = jnp.float32
BF16 = jnp.bfloat16
NT = (((1,), (1,)), ((), ()))
TN = (((0,), (0,)), ((), ()))


MESH = pl.DeviceIdType.MESH


def target(n, i):
    return lax.rem(lax.axis_index("dp") + 2 * i, n)


def mate():
    me = lax.axis_index("dp")
    return me + 1 - 2 * lax.rem(me, 2)


def greet(n):
    barrier = pltpu.get_barrier_semaphore()

    def hello(i, _):
        pl.semaphore_signal(barrier, inc=1, device_id=(target(n, i),), device_id_type=MESH)
        return 0

    pl.semaphore_signal(barrier, inc=1, device_id=(mate(),), device_id_type=MESH)
    lax.fori_loop(1, n // 2, hello, 0)


def each(low, high, act):
    def step(i, _):
        act(i)
        return 0

    lax.fori_loop(low, high, step, 0)


def remote(src, dst, sems, kind, device):
    return pltpu.make_async_remote_copy(
        src_ref=src,
        dst_ref=dst,
        send_sem=sems.at[2 * kind],
        recv_sem=sems.at[2 * kind + 1],
        device_id=(device,),
        device_id_type=MESH,
    )


class Exchange:
    def __init__(self, n, ref, sems):
        self.n, self.ref, self.sems = n, ref, sems
        self.me = lax.axis_index("dp")
        self.half = n // 2

    def own(self):
        return self.ref.at[self.me]

    def several(self, kind, count):
        blocks = self.ref.at[pl.ds(0, count)]
        return remote(blocks, blocks, self.sems, kind, mate())

    def relay(self):
        parity = lax.rem(self.me, 2)
        blocks = self.ref.reshape(self.half, 2, *self.ref.shape[1:]).at[:, parity]
        return remote(blocks, blocks, self.sems, self.last, mate())

    def forward(self):
        self.several(*self.counts[-1]).wait_recv()
        self.relay().start()

    def arrive(self):
        self.relay().wait_recv()

    def drain(self):
        for kind, count in self.counts:
            self.several(kind, count).wait_send()
        self.relay().wait_send()


class Share(Exchange):
    last = 1

    def __init__(self, n, ref, sems):
        super().__init__(n, ref, sems)
        self.counts = ((0, self.half - 1),)

    def start(self):
        own = self.own()
        each(1, self.half, lambda i: remote(own, own, self.sems, 0, target(self.n, i)).start())


class LineShare(Exchange):
    last = 2

    def __init__(self, n, ref, sems):
        super().__init__(n, ref, sems)
        self.lines = line_count(n)
        self.plane = n // self.lines
        self.peers = self.plane // 2
        self.spot = lax.rem(self.me, self.plane)
        self.counts = ((0, self.lines - 1), (1, self.lines * (self.peers - 1)))

    def across(self, j):
        block = self.ref.at[lax.rem(self.me - self.plane * j + self.n, self.n)]

        def send(k):
            device = self.me - self.spot + lax.rem(self.spot + 2 * k, self.plane)
            remote(block, block, self.sems, 1, device).start()

        each(1, self.peers, send)

    def start(self):
        own = self.own()
        for j in range(1, self.lines):
            remote(own, own, self.sems, 0, lax.rem(self.me + self.plane * j, self.n)).start()
        self.across(0)

    def spread(self):
        self.several(*self.counts[0]).wait_recv()
        for j in range(1, self.lines):
            self.across(j)


def line_count(n):
    return 4 if n % 8 == 0 else 1


def embed_kernel(
    n,
    x_hbm,
    gain_hbm,
    wq_hbm,
    wk_hbm,
    wv_hbm,
    wo_hbm,
    text_hbm,
    all_txt,
    abar0,
    abar1,
    abar2,
    emb_ref,
    text_ref,
    xs,
    gain_ref,
    wqks,
    wvs,
    wos,
    normed,
    qkn0,
    qkn1,
    pooled,
    zs,
    xbar,
    all_xbar,
    x_sem,
    q_sem,
    k_sem,
    w_sem,
    share_sems,
):
    images, tokens, width = xs.shape
    groups = wqks.shape[0]
    cols = width // groups
    head = width // HEADS
    me = lax.axis_index("dp")
    abars = (abar0, abar1, abar2)

    def x_copy(i):
        return pltpu.make_async_copy(x_hbm.at[i], xs.at[i], x_sem.at[i])

    def q_copy(g):
        return pltpu.make_async_copy(
            wq_hbm.at[:, pl.ds(g * cols, cols)], wqks.at[g, :, pl.ds(0, cols)], q_sem.at[g]
        )

    def k_copy(g):
        return pltpu.make_async_copy(
            wk_hbm.at[:, pl.ds(g * cols, cols)], wqks.at[g, :, pl.ds(cols, cols)], k_sem.at[g]
        )

    v_copy = pltpu.make_async_copy(wv_hbm, wvs, w_sem.at[0])
    o_copy = pltpu.make_async_copy(wo_hbm, wos, w_sem.at[1])
    gain_copy = pltpu.make_async_copy(gain_hbm, gain_ref, w_sem.at[2])
    text_copy = pltpu.make_async_copy(text_hbm, text_ref, w_sem.at[3])
    gain_copy.start()
    for i in range(images):
        x_copy(i).start()
    text_copy.start()
    greet(n)
    for g in range(groups):
        q_copy(g).start()
        k_copy(g).start()
    v_copy.start()
    o_copy.start()

    txt_share = LineShare(n, all_txt, share_sems.at[0])
    xbar_share = LineShare(n, all_xbar, share_sems.at[1])

    pooled[...] = jnp.zeros_like(pooled)
    gain_copy.wait()
    gain = gain_ref[...]
    block = 32

    def norm_image(i, _):
        x_copy(i).wait()

        def norm_block(b, acc):
            x = xs[i, pl.ds(b * block, block), :].astype(F32)
            center = x - jnp.mean(x, axis=-1, keepdims=True)
            spread = jnp.mean(center * center, axis=-1, keepdims=True)
            out = center * lax.rsqrt(spread + epsilon) * gain
            rows = pl.ds(pl.multiple_of(i * tokens + b * block, block), block)
            normed[rows, :] = out.astype(BF16)
            return acc + jnp.sum(x, axis=0, keepdims=True)

        total = lax.fori_loop(0, tokens // block, norm_block, jnp.zeros((1, width), F32), unroll=4)
        first = xs[i, pl.ds(0, 1), :].astype(F32)
        xbar[pl.ds(i, 1), :] = first + (total - first) / (tokens - 1)
        return 0

    lax.fori_loop(0, images, norm_image, 0)
    all_xbar[me] = xbar[...].astype(BF16)
    text_copy.wait()
    text32 = text_ref[...].astype(F32)
    txt_norm = jnp.sqrt(jnp.sum(text32 * text32, axis=1, keepdims=True) + epsilon)
    all_txt[me] = (text32 / txt_norm).astype(BF16)

    seg_row = lax.broadcasted_iota(jnp.int32, (cols, cols), 0) // head
    seg_col = lax.broadcasted_iota(jnp.int32, (cols, cols), 1) // head
    seg = jnp.where(seg_row == seg_col, 1.0, 0.0).astype(BF16)
    lanes = 128
    per = lanes // head
    lane_head = lax.broadcasted_iota(jnp.int32, (tokens, lanes), 1) // head
    coef = jnp.where(
        lax.broadcasted_iota(jnp.int32, (tokens, 1), 0) == 0, 1.0, 1.0 / (tokens - 1)
    ).astype(F32)

    def unit(proj):
        sq = jnp.dot((proj * proj).astype(BF16), seg, preferred_element_type=F32)
        return (proj * lax.rsqrt(sq + epsilon)).astype(BF16)

    qkns = (qkn0, qkn1)

    def project(g, b):
        rows = pl.ds(b * (images * tokens // BLOCKS), images * tokens // BLOCKS)
        proj = jnp.dot(normed[rows, :], wqks[g], preferred_element_type=F32)
        qkn = qkns[g % 2]
        qkn[rows, 0:cols] = unit(proj[:, 0:cols])
        qkn[rows, cols : 2 * cols] = unit(proj[:, cols : 2 * cols])

    def attend(g, i):
        rows = pl.ds(i * tokens, tokens)
        qkn = qkns[g % 2]
        for pair in range(cols // lanes):
            lo = pair * lanes
            qi = qkn[rows, lo : lo + lanes]
            ki = qkn[rows, cols + lo : cols + lo + lanes]
            km = jnp.concatenate(
                [jnp.where(lane_head == h, ki, jnp.zeros_like(ki)) for h in range(per)],
                axis=0,
            )
            s = lax.dot_general(qi, km, NT, preferred_element_type=F32)
            e = jnp.exp2(s * (attn_temp * log2e))
            for h in range(per):
                eh = e[:, h * tokens : (h + 1) * tokens]
                scale = coef / jnp.sum(eh, axis=-1, keepdims=True)
                ph = jnp.sum(eh * scale, axis=0, keepdims=True)
                at = g * SLOTS + pair * per + h
                pooled[i, at : at + 1, :] = ph

    def weigh(low, high):
        rows = SLOTS * (high - low)
        wide = cols * (high - low)
        for i in range(images):
            p = pooled[i, low * SLOTS : high * SLOTS, :]
            hi = p.astype(BF16)
            lo = (p - hi.astype(F32)).astype(BF16)
            z2 = jnp.dot(
                jnp.concatenate([hi, lo], axis=0),
                normed[i * tokens : (i + 1) * tokens, :],
                preferred_element_type=F32,
            )
            z = z2[:rows] + z2[rows:]
            hi = z.astype(BF16)
            zs[0, i * rows : (i + 1) * rows, :] = hi
            zs[1, i * rows : (i + 1) * rows, :] = (z - hi.astype(F32)).astype(BF16)
        wv = wvs[:, low * cols : high * cols]
        full = jnp.dot(zs[0, : images * rows, :], wv, preferred_element_type=F32) + jnp.dot(
            zs[1, : images * rows, :], wv, preferred_element_type=F32
        )
        slot = lax.broadcasted_iota(jnp.int32, (rows, wide), 0)
        owner = lax.broadcasted_iota(jnp.int32, (rows, wide), 1) // head
        keep = slot == owner // GROUP * SLOTS + owner % GROUP
        picked = [
            jnp.sum(
                jnp.where(keep, full[i * rows : (i + 1) * rows, :], 0.0), axis=0, keepdims=True
            )
            for i in range(images)
        ]
        return jnp.concatenate(picked, axis=0).astype(BF16)

    early, late, last = groups // 2, groups - 1, groups
    shares = [Share(n, part, share_sems.at[2 + c]) for c, part in enumerate(abars)]
    for g in range(groups + 1):
        if g < groups:
            q_copy(g).wait()
            k_copy(g).wait()
        if g == 1:
            pl.semaphore_wait(pltpu.get_barrier_semaphore(), n // 2)
            txt_share.start()
            xbar_share.start()
        if g == early + 1:
            txt_share.spread()
            v_copy.wait()
            abars[0][me] = weigh(0, early)
            shares[0].start()
        if g == groups:
            xbar_share.spread()
            abars[1][me] = weigh(early, late)
        for b in range(BLOCKS):
            if g > 0:
                for i in range(b * images // BLOCKS, (b + 1) * images // BLOCKS):
                    attend(g - 1, i)
            if g < groups:
                project(g, b)
    shares[1].start()
    abars[2][me] = weigh(late, last)
    shares[2].start()
    txt_share.forward()
    xbar_share.forward()
    shares[0].forward()
    shares[1].forward()
    xbar_share.arrive()
    shares[0].arrive()
    o_copy.wait()

    total = n * images
    chunk = min(total, 256)
    part = chunk // images

    def join(ref, r):
        return ref[r * part : (r + 1) * part].reshape(chunk, ref.shape[-1])

    def out_part(r, c, low, high):
        w = wos[low * cols : high * cols, :]
        return jnp.dot(join(abars[c], r), w, preferred_element_type=F32)

    for r in range(total // chunk):
        emb = join(all_xbar, r).astype(F32) + out_part(r, 0, 0, early)
        emb_ref[r * chunk : (r + 1) * chunk, :] = emb
    shares[2].forward()
    txt_share.arrive()
    shares[1].arrive()
    for share in (txt_share, xbar_share, *shares):
        if share is not shares[2]:
            share.drain()
    shares[2].arrive()
    for r in range(total // chunk):
        emb_ref[r * chunk : (r + 1) * chunk, :] += out_part(r, 1, early, late) + out_part(
            r, 2, late, last
        )
    shares[2].drain()


def embed(features, ln_gain, w_query, w_key, w_value, w_out, text_raw, n):
    images, tokens, width = features.shape
    groups = HEADS // GROUP
    cols = width // groups
    hbm = pl.BlockSpec(memory_space=pl.ANY)
    vmem = pl.BlockSpec(memory_space=pltpu.VMEM)
    args = (features, ln_gain.reshape(1, width), w_query, w_key, w_value, w_out, text_raw)
    args = [pltpu.with_memory_space_constraint(a, pltpu.HBM) for a in args]
    return pl.pallas_call(
        functools.partial(embed_kernel, n),
        out_shape=(
            pltpu.VMEM((n, images, width), BF16),
            pltpu.VMEM((n, images, width // 2), BF16),
            pltpu.VMEM((n, images, width // 4), BF16),
            pltpu.VMEM((n, images, width // 4), BF16),
            pltpu.VMEM((n * images, width), F32),
            pltpu.VMEM((images, width), BF16),
        ),
        in_specs=[hbm] * 7,
        out_specs=(vmem,) * 6,
        scratch_shapes=[
            pltpu.VMEM((images, tokens, width), BF16),
            pltpu.VMEM((1, width), F32),
            pltpu.VMEM((groups, width, 2 * cols), BF16),
            pltpu.VMEM((width, width), BF16),
            pltpu.VMEM((width, width), BF16),
            pltpu.VMEM((images * tokens, width), BF16),
            pltpu.VMEM((images * tokens, 2 * cols), BF16),
            pltpu.VMEM((images * tokens, 2 * cols), BF16),
            pltpu.VMEM((images, SLOTS * groups, tokens), F32),
            pltpu.VMEM((2, images * SLOTS * groups, width), BF16),
            pltpu.VMEM((images, width), F32),
            pltpu.VMEM((n, images, width), BF16),
            pltpu.SemaphoreType.DMA((images,)),
            pltpu.SemaphoreType.DMA((groups,)),
            pltpu.SemaphoreType.DMA((groups,)),
            pltpu.SemaphoreType.DMA((4,)),
            pltpu.SemaphoreType.DMA((5, 6)),
        ],
        compiler_params=pltpu.CompilerParams(
            collective_id=0, has_side_effects=True, vmem_limit_bytes=40 * 2**20
        ),
        name="embed",
    )(*args)


def loss_kernel(
    txt_ref, abar0, abar1, abar2, emb_ref, text_ref, loss_ref, text_grad_ref, w_hbm, img_s, grad_s, w_s, w_sem
):
    total, width = emb_ref.shape
    images = text_ref.shape[0]
    chunk = min(total, 256)
    chunks = [slice(r, r + chunk) for r in range(0, total, chunk)]

    def eye(r):
        row = lax.broadcasted_iota(jnp.int32, (chunk, total), 0) + r.start
        return row == lax.broadcasted_iota(jnp.int32, (chunk, total), 1)

    txt = txt_ref[...]
    invs, es, rowsums = [], [], []
    colsum = rowsum_flat = jnp.zeros((1, total), F32)
    diag = jnp.zeros((1, total), F32)
    for r in chunks:
        emb = emb_ref[r, :]
        inv = lax.rsqrt(jnp.sum(emb * emb, axis=1, keepdims=True) + epsilon)
        img = (emb * inv).astype(BF16)
        img_s[r, :] = img
        logits = inv_temp * lax.dot_general(img, txt, NT, preferred_element_type=F32)
        e = jnp.exp(logits)
        rowsum = jnp.sum(e, axis=1, keepdims=True)
        colsum = colsum + jnp.sum(e, axis=0, keepdims=True)
        rowsum_flat = rowsum_flat + jnp.sum(jnp.where(eye(r), rowsum, 0.0), axis=0, keepdims=True)
        diag = diag + jnp.sum(jnp.where(eye(r), logits, 0.0), axis=0, keepdims=True)
        invs.append(inv)
        es.append(e)
        rowsums.append(rowsum)

    half_col = 0.5 / colsum
    for r, inv, e, rowsum in zip(chunks, invs, es, rowsums):
        delta = e * (0.5 / rowsum + half_col) - jnp.where(eye(r), 1.0, 0.0)
        grad = jnp.dot(delta.astype(BF16), txt, preferred_element_type=F32)
        emb = emb_ref[r, :]
        along = jnp.sum(emb * grad, axis=1, keepdims=True) * (inv * inv)
        grad_s[r, :] = ((grad - emb * along) * (inv_temp * inv)).astype(BF16)

    rows = width // w_sem.shape[0]

    def abar(low, wide):
        for ref in (abar0, abar1, abar2):
            if low < ref.shape[1]:
                return ref[:, low : low + wide]
            low -= ref.shape[1]

    def w_copy(c):
        return pltpu.make_async_copy(
            w_s.at[pl.ds(c * rows, rows), :], w_hbm.at[pl.ds(c * rows, rows), :], w_sem.at[c]
        )

    for c in range(w_sem.shape[0]):
        w_s[c * rows : (c + 1) * rows, :] = lax.dot_general(
            abar(c * rows, rows), grad_s[...], TN, preferred_element_type=F32
        ).astype(BF16)
        w_copy(c).start()

    loss_ref[0, 0] = jnp.sum(
        jnp.log(rowsum_flat) + jnp.log(colsum) - 2.0 * diag
    ) / (2.0 * total)

    img = img_s[...]
    text32 = text_ref[...].astype(F32)
    txt_norm = jnp.sqrt(jnp.sum(text32 * text32, axis=1, keepdims=True) + epsilon)
    txt_f = text32 / txt_norm
    own = inv_temp * lax.dot_general(txt_f.astype(BF16), img, NT, preferred_element_type=F32)
    own_e = jnp.exp(own)
    own_sum = jnp.sum(own_e, axis=1, keepdims=True)
    col = lax.broadcasted_iota(jnp.int32, (images, total), 1)
    row = lax.broadcasted_iota(jnp.int32, (images, total), 0) + lax.axis_index("dp") * images
    own_delta = 0.5 * (own_e / rowsum_flat + own_e / own_sum) - jnp.where(col == row, 1.0, 0.0)
    grad_txt = inv_temp * jnp.dot(own_delta.astype(BF16), img, preferred_element_type=F32)
    text_grad_ref[...] = (
        grad_txt - txt_f * jnp.sum(txt_f * grad_txt, axis=1, keepdims=True)
    ) / txt_norm
    for c in range(w_sem.shape[0]):
        w_copy(c).wait()


def finish(all_txt, abars, emb, text_raw):
    images, width = text_raw.shape
    total = emb.shape[0]
    vmem = pl.BlockSpec(memory_space=pltpu.VMEM)
    smem = pl.BlockSpec(memory_space=pltpu.SMEM)
    loss, text_grad, w_grad = pl.pallas_call(
        loss_kernel,
        out_shape=(
            jax.ShapeDtypeStruct((1, 1), F32),
            jax.ShapeDtypeStruct((images, width), F32),
            jax.ShapeDtypeStruct((width, width), BF16),
        ),
        in_specs=[vmem] * 6,
        out_specs=(smem, vmem, pl.BlockSpec(memory_space=pl.ANY)),
        scratch_shapes=[
            pltpu.VMEM((total, width), BF16),
            pltpu.VMEM((total, width), BF16),
            pltpu.VMEM((width, width), BF16),
            pltpu.SemaphoreType.DMA((4,)),
        ],
        compiler_params=pltpu.CompilerParams(vmem_limit_bytes=40 * 2**20),
        name="finish",
    )(all_txt, *abars, emb, text_raw)
    return loss.reshape(()), text_grad, w_grad


def solution(mesh):
    n = mesh.shape["dp"]

    def local(features, ln_gain, w_query, w_key, w_value, w_out, text_raw):
        all_txt, *abars, emb, text = embed(
            features, ln_gain, w_query, w_key, w_value, w_out, text_raw, n
        )
        pairs = n * text_raw.shape[0]
        abars = [a.reshape(pairs, -1) for a in abars]
        return finish(all_txt.reshape(pairs, -1), abars, emb, text)

    placed = (P("dp", None, None), P(), P(), P(), P(), P(), P("dp", None))
    return jax.shard_map(
        local, mesh=mesh, in_specs=placed, out_specs=(P(), P("dp", None), P()), check_vma=False
    )
```

```python
import functools

import jax
import jax.numpy as jnp
from jax import lax
from jax.experimental import pallas as pl
from jax.experimental.pallas import tpu as pltpu
from jax.sharding import PartitionSpec as P

HEADS = 16
GROUP = 4
BLOCKS = 2
SLOTS = 8

inv_temp = 1.0 / 0.07
attn_temp = 8.0
epsilon = 1e-06
log2e = 1.4426950408889634

F32 = jnp.float32
BF16 = jnp.bfloat16
NT = (((1,), (1,)), ((), ()))
TN = (((0,), (0,)), ((), ()))


MESH = pl.DeviceIdType.MESH


def target(n, i):
    return lax.rem(lax.axis_index("dp") + 2 * i, n)


def mate():
    me = lax.axis_index("dp")
    return me + 1 - 2 * lax.rem(me, 2)


def greet(n):
    barrier = pltpu.get_barrier_semaphore()
    me = lax.axis_index("dp")

    def hello(i, _):
        pl.semaphore_signal(
            barrier, inc=1, device_id=(lax.rem(me + i, n),), device_id_type=MESH
        )
        return 0

    lax.fori_loop(1, n, hello, 0)


def each(low, high, act):
    def step(i, _):
        act(i)
        return 0

    lax.fori_loop(low, high, step, 0)


def remote(src, dst, sems, kind, device):
    return pltpu.make_async_remote_copy(
        src_ref=src,
        dst_ref=dst,
        send_sem=sems.at[2 * kind],
        recv_sem=sems.at[2 * kind + 1],
        device_id=(device,),
        device_id_type=MESH,
    )


class Exchange:
    def __init__(self, n, ref, sems):
        self.n, self.ref, self.sems = n, ref, sems
        self.me = lax.axis_index("dp")
        self.half = n // 2

    def own(self):
        return self.ref.at[self.me]

    def several(self, kind, count):
        blocks = self.ref.at[pl.ds(0, count)]
        return remote(blocks, blocks, self.sems, kind, mate())

    def relay(self):
        parity = lax.rem(self.me, 2)
        blocks = self.ref.reshape(self.half, 2, *self.ref.shape[1:]).at[:, parity]
        return remote(blocks, blocks, self.sems, self.last, mate())

    def forward(self):
        self.several(*self.counts[-1]).wait_recv()
        self.relay().start()

    def arrive(self):
        self.relay().wait_recv()

    def drain(self):
        for kind, count in self.counts:
            self.several(kind, count).wait_send()
        self.relay().wait_send()


class Share(Exchange):
    last = 1

    def __init__(self, n, ref, sems):
        super().__init__(n, ref, sems)
        self.counts = ((0, self.half - 1),)

    def start(self):
        own = self.own()
        each(1, self.half, lambda i: remote(own, own, self.sems, 0, target(self.n, i)).start())


class Scatter(Exchange):
    def start(self):
        own = self.own()

        def send(i):
            remote(own, own, self.sems, 0, lax.rem(self.me + i, self.n)).start()

        each(1, self.n, send)

    def arrive(self):
        self.several(0, self.n - 1).wait_recv()

    def drain(self):
        self.several(0, self.n - 1).wait_send()


class LineShare(Exchange):
    last = 2

    def __init__(self, n, ref, sems):
        super().__init__(n, ref, sems)
        self.lines = line_count(n)
        self.plane = n // self.lines
        self.peers = self.plane // 2
        self.spot = lax.rem(self.me, self.plane)
        self.counts = ((0, self.lines - 1), (1, self.lines * (self.peers - 1)))

    def across(self, j):
        block = self.ref.at[lax.rem(self.me - self.plane * j + self.n, self.n)]

        def send(k):
            device = self.me - self.spot + lax.rem(self.spot + 2 * k, self.plane)
            remote(block, block, self.sems, 1, device).start()

        each(1, self.peers, send)

    def start(self):
        own = self.own()
        for j in range(1, self.lines):
            remote(own, own, self.sems, 0, lax.rem(self.me + self.plane * j, self.n)).start()
        self.across(0)

    def spread(self):
        self.several(*self.counts[0]).wait_recv()
        for j in range(1, self.lines):
            self.across(j)


def line_count(n):
    return 4 if n % 8 == 0 else 1


def embed_kernel(
    n,
    x_hbm,
    gain_hbm,
    wq_hbm,
    wk_hbm,
    wv_hbm,
    wo_hbm,
    text_hbm,
    all_txt,
    abar0,
    abar1,
    abar2,
    emb_ref,
    text_ref,
    xs,
    gain_ref,
    wqks,
    wvs,
    wos,
    normed,
    qkn0,
    qkn1,
    pooled,
    zs,
    xbar,
    all_xbar,
    x_sem,
    q_sem,
    k_sem,
    w_sem,
    share_sems,
):
    images, tokens, width = xs.shape
    groups = wqks.shape[0]
    cols = width // groups
    head = width // HEADS
    me = lax.axis_index("dp")
    abars = (abar0, abar1, abar2)

    def x_copy(i):
        return pltpu.make_async_copy(x_hbm.at[i], xs.at[i], x_sem.at[i])

    def q_copy(g):
        return pltpu.make_async_copy(
            wq_hbm.at[:, pl.ds(g * cols, cols)], wqks.at[g, :, pl.ds(0, cols)], q_sem.at[g]
        )

    def k_copy(g):
        return pltpu.make_async_copy(
            wk_hbm.at[:, pl.ds(g * cols, cols)], wqks.at[g, :, pl.ds(cols, cols)], k_sem.at[g]
        )

    v_copy = pltpu.make_async_copy(wv_hbm, wvs, w_sem.at[0])
    o_copy = pltpu.make_async_copy(wo_hbm, wos, w_sem.at[1])
    gain_copy = pltpu.make_async_copy(gain_hbm, gain_ref, w_sem.at[2])
    text_copy = pltpu.make_async_copy(text_hbm, text_ref, w_sem.at[3])
    gain_copy.start()
    for i in range(images):
        x_copy(i).start()
    text_copy.start()
    greet(n)
    for g in range(groups):
        q_copy(g).start()
        k_copy(g).start()
    v_copy.start()
    o_copy.start()

    txt_share = LineShare(n, all_txt, share_sems.at[0])
    xbar_share = LineShare(n, all_xbar, share_sems.at[1])

    pooled[...] = jnp.zeros_like(pooled)
    gain_copy.wait()
    gain = gain_ref[...]
    block = 32

    def norm_block(i, b, acc):
        x = xs[i, pl.ds(b * block, block), :].astype(F32)
        center = x - jnp.mean(x, axis=-1, keepdims=True)
        spread = jnp.mean(center * center, axis=-1, keepdims=True)
        out = center * lax.rsqrt(spread + epsilon) * gain
        rows = pl.ds(pl.multiple_of(i * tokens + b * block, block), block)
        normed[rows, :] = out.astype(BF16)
        return acc + jnp.sum(x, axis=0, keepdims=True)

    def mean_tokens(i, total):
        first = xs[i, pl.ds(0, 1), :].astype(F32)
        xbar[pl.ds(i, 1), :] = first + (total - first) / (tokens - 1)

    def norm_image(i, _):
        x_copy(i).wait()
        zero = jnp.zeros((1, width), F32)
        total = lax.fori_loop(
            0, tokens // block, lambda b, acc: norm_block(i, b, acc), zero, unroll=4
        )
        mean_tokens(i, total)
        return 0

    ahead = images // BLOCKS
    lax.fori_loop(0, ahead, norm_image, 0)
    seg_row = lax.broadcasted_iota(jnp.int32, (cols, cols), 0) // head
    seg_col = lax.broadcasted_iota(jnp.int32, (cols, cols), 1) // head
    seg = jnp.where(seg_row == seg_col, 1.0, 0.0).astype(BF16)
    lanes = 128
    per = lanes // head
    lane_head = lax.broadcasted_iota(jnp.int32, (tokens, lanes), 1) // head
    coef = jnp.where(
        lax.broadcasted_iota(jnp.int32, (tokens, 1), 0) == 0, 1.0, 1.0 / (tokens - 1)
    ).astype(F32)

    def unit(proj):
        sq = jnp.dot((proj * proj).astype(BF16), seg, preferred_element_type=F32)
        return (proj * lax.rsqrt(sq + epsilon)).astype(BF16)

    qkns = (qkn0, qkn1)

    def project(g, b):
        rows = pl.ds(b * (images * tokens // BLOCKS), images * tokens // BLOCKS)
        proj = jnp.dot(normed[rows, :], wqks[g], preferred_element_type=F32)
        qkn = qkns[g % 2]
        qkn[rows, 0:cols] = unit(proj[:, 0:cols])
        qkn[rows, cols : 2 * cols] = unit(proj[:, cols : 2 * cols])

    def attend(g, i):
        rows = pl.ds(i * tokens, tokens)
        qkn = qkns[g % 2]
        for pair in range(cols // lanes):
            lo = pair * lanes
            qi = qkn[rows, lo : lo + lanes]
            ki = qkn[rows, cols + lo : cols + lo + lanes]
            km = jnp.concatenate(
                [jnp.where(lane_head == h, ki, jnp.zeros_like(ki)) for h in range(per)],
                axis=0,
            )
            s = lax.dot_general(qi, km, NT, preferred_element_type=F32)
            e = jnp.exp2(s * (attn_temp * log2e))
            for h in range(per):
                eh = e[:, h * tokens : (h + 1) * tokens]
                scale = coef / jnp.sum(eh, axis=-1, keepdims=True)
                ph = jnp.sum(eh * scale, axis=0, keepdims=True)
                at = g * SLOTS + pair * per + h
                pooled[i, at : at + 1, :] = ph

    def weigh(low, high):
        rows = SLOTS * (high - low)
        wide = cols * (high - low)
        for i in range(images):
            p = pooled[i, low * SLOTS : high * SLOTS, :]
            hi = p.astype(BF16)
            lo = (p - hi.astype(F32)).astype(BF16)
            z2 = jnp.dot(
                jnp.concatenate([hi, lo], axis=0),
                normed[i * tokens : (i + 1) * tokens, :],
                preferred_element_type=F32,
            )
            z = z2[:rows] + z2[rows:]
            hi = z.astype(BF16)
            zs[0, i * rows : (i + 1) * rows, :] = hi
            zs[1, i * rows : (i + 1) * rows, :] = (z - hi.astype(F32)).astype(BF16)
        wv = wvs[:, low * cols : high * cols]
        full = jnp.dot(zs[0, : images * rows, :], wv, preferred_element_type=F32) + jnp.dot(
            zs[1, : images * rows, :], wv, preferred_element_type=F32
        )
        slot = lax.broadcasted_iota(jnp.int32, (rows, wide), 0)
        owner = lax.broadcasted_iota(jnp.int32, (rows, wide), 1) // head
        keep = slot == owner // GROUP * SLOTS + owner % GROUP
        picked = [
            jnp.sum(
                jnp.where(keep, full[i * rows : (i + 1) * rows, :], 0.0), axis=0, keepdims=True
            )
            for i in range(images)
        ]
        return jnp.concatenate(picked, axis=0).astype(BF16)

    early, late, last = groups // 2, groups - 1, groups
    kinds = (Share, Share, Scatter)
    shares = [kinds[c](n, part, share_sems.at[2 + c]) for c, part in enumerate(abars)]
    for g in range(groups + 1):
        if g < groups:
            q_copy(g).wait()
            k_copy(g).wait()
        if g == 1:
            pl.semaphore_wait(pltpu.get_barrier_semaphore(), n - 1)
            xbar_share.start()
            txt_share.start()
        if g == early + 1:
            v_copy.wait()
            abars[0][me] = weigh(0, early)
            shares[0].start()
            xbar_share.spread()
        if g == groups:
            txt_share.spread()
            abars[1][me] = weigh(early, late)
        if g == 0:
            for i in range(ahead, images):
                x_copy(i).wait()
            for i in range(ahead, images):
                total = jnp.zeros((1, width), F32)
                for b in range(tokens // block):
                    total = norm_block(i, b, total)
                mean_tokens(i, total)
            project(0, 0)
            for b in range(1, BLOCKS):
                project(0, b)
            all_xbar[me] = xbar[...].astype(BF16)
            text_copy.wait()
            text32 = text_ref[...].astype(F32)
            txt_norm = jnp.sqrt(jnp.sum(text32 * text32, axis=1, keepdims=True) + epsilon)
            all_txt[me] = (text32 / txt_norm).astype(BF16)
            continue
        for b in range(BLOCKS):
            if g > 0:
                for i in range(b * images // BLOCKS, (b + 1) * images // BLOCKS):
                    attend(g - 1, i)
            if g < groups:
                project(g, b)
    shares[1].start()
    abars[2][me] = weigh(late, last)
    shares[2].start()
    xbar_share.forward()
    shares[0].forward()
    shares[1].forward()
    txt_share.forward()
    o_copy.wait()

    total = n * images
    chunk = min(total, 256)
    part = chunk // images

    def join(ref, r):
        return ref[r * part : (r + 1) * part].reshape(chunk, ref.shape[-1])

    def out_part(r, c, low, high):
        w = wos[low * cols : high * cols, :]
        return jnp.dot(join(abars[c], r), w, preferred_element_type=F32)

    for share in (xbar_share, shares[0]):
        share.arrive()
        share.drain()
    for r in range(total // chunk):
        emb = join(all_xbar, r).astype(F32) + out_part(r, 0, 0, early)
        emb_ref[r * chunk : (r + 1) * chunk, :] = emb
    for share in (shares[1], shares[2]):
        share.arrive()
    for r in range(total // chunk):
        emb_ref[r * chunk : (r + 1) * chunk, :] += out_part(r, 1, early, late) + out_part(
            r, 2, late, last
        )
    txt_share.arrive()
    for share in (txt_share, shares[1], shares[2]):
        share.drain()


def embed(features, ln_gain, w_query, w_key, w_value, w_out, text_raw, n):
    images, tokens, width = features.shape
    groups = HEADS // GROUP
    cols = width // groups
    hbm = pl.BlockSpec(memory_space=pl.ANY)
    vmem = pl.BlockSpec(memory_space=pltpu.VMEM)
    args = (features, ln_gain.reshape(1, width), w_query, w_key, w_value, w_out, text_raw)
    args = [pltpu.with_memory_space_constraint(a, pltpu.HBM) for a in args]
    return pl.pallas_call(
        functools.partial(embed_kernel, n),
        out_shape=(
            pltpu.VMEM((n, images, width), BF16),
            pltpu.VMEM((n, images, width // 2), BF16),
            pltpu.VMEM((n, images, width // 4), BF16),
            pltpu.VMEM((n, images, width // 4), BF16),
            pltpu.VMEM((n * images, width), F32),
            pltpu.VMEM((images, width), BF16),
        ),
        in_specs=[hbm] * 7,
        out_specs=(vmem,) * 6,
        scratch_shapes=[
            pltpu.VMEM((images, tokens, width), BF16),
            pltpu.VMEM((1, width), F32),
            pltpu.VMEM((groups, width, 2 * cols), BF16),
            pltpu.VMEM((width, width), BF16),
            pltpu.VMEM((width, width), BF16),
            pltpu.VMEM((images * tokens, width), BF16),
            pltpu.VMEM((images * tokens, 2 * cols), BF16),
            pltpu.VMEM((images * tokens, 2 * cols), BF16),
            pltpu.VMEM((images, SLOTS * groups, tokens), F32),
            pltpu.VMEM((2, images * SLOTS * groups, width), BF16),
            pltpu.VMEM((images, width), F32),
            pltpu.VMEM((n, images, width), BF16),
            pltpu.SemaphoreType.DMA((images,)),
            pltpu.SemaphoreType.DMA((groups,)),
            pltpu.SemaphoreType.DMA((groups,)),
            pltpu.SemaphoreType.DMA((4,)),
            pltpu.SemaphoreType.DMA((5, 6)),
        ],
        compiler_params=pltpu.CompilerParams(
            collective_id=0, has_side_effects=True, vmem_limit_bytes=40 * 2**20
        ),
        name="embed",
    )(*args)


def loss_kernel(
    txt_ref,
    abar0,
    abar1,
    abar2,
    emb_ref,
    text_ref,
    loss_hbm,
    text_grad_hbm,
    w_hbm,
    img_s,
    grad_s,
    w_s,
    loss_s,
    text_grad_s,
    out_sem,
):
    total, width = emb_ref.shape
    images = text_ref.shape[0]
    chunk = min(total, 256)
    chunks = [slice(r, r + chunk) for r in range(0, total, chunk)]
    pieces = 4
    rows = width // pieces

    def w_copy(c):
        return pltpu.make_async_copy(
            w_s.at[pl.ds(c * rows, rows), :], w_hbm.at[pl.ds(c * rows, rows), :], out_sem.at[c]
        )

    loss_copy = pltpu.make_async_copy(loss_s, loss_hbm, out_sem.at[pieces])
    text_copy = pltpu.make_async_copy(text_grad_s, text_grad_hbm, out_sem.at[pieces + 1])

    def eye(r):
        row = lax.broadcasted_iota(jnp.int32, (chunk, total), 0) + r.start
        return row == lax.broadcasted_iota(jnp.int32, (chunk, total), 1)

    def abar(low, wide):
        for ref in (abar0, abar1, abar2):
            if low < ref.shape[1]:
                return ref[:, low : low + wide]
            low -= ref.shape[1]

    txt = txt_ref[...]
    invs, es, rowsums = [], [], []
    colsum = rowsum_flat = jnp.zeros((1, total), F32)
    diag = jnp.zeros((1, total), F32)
    for r in chunks:
        emb = emb_ref[r, :]
        inv = lax.rsqrt(jnp.sum(emb * emb, axis=1, keepdims=True) + epsilon)
        img = (emb * inv).astype(BF16)
        img_s[r, :] = img
        logits = inv_temp * lax.dot_general(img, txt, NT, preferred_element_type=F32)
        e = jnp.exp(logits)
        rowsum = jnp.sum(e, axis=1, keepdims=True)
        colsum = colsum + jnp.sum(e, axis=0, keepdims=True)
        rowsum_flat = rowsum_flat + jnp.sum(jnp.where(eye(r), rowsum, 0.0), axis=0, keepdims=True)
        diag = diag + jnp.sum(jnp.where(eye(r), logits, 0.0), axis=0, keepdims=True)
        invs.append(inv)
        es.append(e)
        rowsums.append(rowsum)

    half_col = 0.5 / colsum
    text32 = text_ref[...].astype(F32)
    txt_norm = jnp.sqrt(jnp.sum(text32 * text32, axis=1, keepdims=True) + epsilon)
    txt_f = text32 / txt_norm
    img = img_s[...]
    own = inv_temp * lax.dot_general(txt_f.astype(BF16), img, NT, preferred_element_type=F32)

    for r, inv, e, rowsum in zip(chunks, invs, es, rowsums):
        delta = e * (0.5 / rowsum + half_col) - jnp.where(eye(r), 1.0, 0.0)
        grad = jnp.dot(delta.astype(BF16), txt, preferred_element_type=F32)
        emb = emb_ref[r, :]
        along = jnp.sum(emb * grad, axis=1, keepdims=True) * (inv * inv)
        grad_s[r, :] = ((grad - emb * along) * (inv_temp * inv)).astype(BF16)

    loss = jnp.sum(jnp.log(rowsum_flat) + jnp.log(colsum) - 2.0 * diag, axis=1, keepdims=True)
    loss_s[...] = loss / (2.0 * total)
    own_e = jnp.exp(own)
    own_sum = jnp.sum(own_e, axis=1, keepdims=True)
    col = lax.broadcasted_iota(jnp.int32, (images, total), 1)
    row = lax.broadcasted_iota(jnp.int32, (images, total), 0) + lax.axis_index("dp") * images
    own_delta = 0.5 * (own_e / rowsum_flat + own_e / own_sum) - jnp.where(col == row, 1.0, 0.0)
    grad_txt = inv_temp * jnp.dot(own_delta.astype(BF16), img, preferred_element_type=F32)
    text_grad_s[...] = (
        grad_txt - txt_f * jnp.sum(txt_f * grad_txt, axis=1, keepdims=True)
    ) / txt_norm

    for c in range(pieces):
        w_s[c * rows : (c + 1) * rows, :] = lax.dot_general(
            abar(c * rows, rows), grad_s[...], TN, preferred_element_type=F32
        ).astype(BF16)
        w_copy(c).start()
        if c == 0:
            loss_copy.start()
            text_copy.start()
    for c in range(pieces):
        w_copy(c).wait()
    loss_copy.wait()
    text_copy.wait()


def finish(all_txt, abars, emb, text_raw):
    images, width = text_raw.shape
    total = emb.shape[0]
    vmem = pl.BlockSpec(memory_space=pltpu.VMEM)
    hbm = pl.BlockSpec(memory_space=pl.ANY)
    loss, text_grad, w_grad = pl.pallas_call(
        loss_kernel,
        out_shape=(
            jax.ShapeDtypeStruct((1, 1), F32),
            jax.ShapeDtypeStruct((images, width), F32),
            jax.ShapeDtypeStruct((width, width), BF16),
        ),
        in_specs=[vmem] * 6,
        out_specs=(hbm,) * 3,
        scratch_shapes=[
            pltpu.VMEM((total, width), BF16),
            pltpu.VMEM((total, width), BF16),
            pltpu.VMEM((width, width), BF16),
            pltpu.VMEM((1, 1), F32),
            pltpu.VMEM((images, width), F32),
            pltpu.SemaphoreType.DMA((6,)),
        ],
        compiler_params=pltpu.CompilerParams(vmem_limit_bytes=40 * 2**20),
        name="finish",
    )(all_txt, *abars, emb, text_raw)
    return loss.reshape(()), text_grad, w_grad


def solution(mesh):
    n = mesh.shape["dp"]

    def local(features, ln_gain, w_query, w_key, w_value, w_out, text_raw):
        all_txt, *abars, emb, text = embed(
            features, ln_gain, w_query, w_key, w_value, w_out, text_raw, n
        )
        pairs = n * text_raw.shape[0]
        abars = [a.reshape(pairs, -1) for a in abars]
        return finish(all_txt.reshape(pairs, -1), abars, emb, text)

    placed = (P("dp", None, None), P(), P(), P(), P(), P(), P("dp", None))
    return jax.shard_map(
        local, mesh=mesh, in_specs=placed, out_specs=(P(), P("dp", None), P()), check_vma=False
    )
```

```python
import functools

import jax
import jax.numpy as jnp
from jax import lax
from jax.experimental import pallas as pl
from jax.experimental.pallas import tpu as pltpu
from jax.sharding import PartitionSpec as P

HEADS = 16
GROUP = 4
BLOCKS = 2
SLOTS = 8

inv_temp = 1.0 / 0.07
attn_temp = 8.0
epsilon = 1e-06
log2e = 1.4426950408889634

F32 = jnp.float32
BF16 = jnp.bfloat16
NT = (((1,), (1,)), ((), ()))
TN = (((0,), (0,)), ((), ()))


MESH = pl.DeviceIdType.MESH


def target(n, i):
    return lax.rem(lax.axis_index("dp") + 2 * i, n)


def mate():
    me = lax.axis_index("dp")
    return me + 1 - 2 * lax.rem(me, 2)


def greet(n):
    barrier = pltpu.get_barrier_semaphore()
    me = lax.axis_index("dp")

    def hello(i, _):
        pl.semaphore_signal(
            barrier, inc=1, device_id=(lax.rem(me + i, n),), device_id_type=MESH
        )
        return 0

    lax.fori_loop(1, n, hello, 0)


def each(low, high, act, unroll=1):
    def step(i, _):
        act(i)
        return 0

    lax.fori_loop(low, high, step, 0, unroll=unroll)


def remote(src, dst, sems, kind, device):
    return pltpu.make_async_remote_copy(
        src_ref=src,
        dst_ref=dst,
        send_sem=sems.at[2 * kind],
        recv_sem=sems.at[2 * kind + 1],
        device_id=(device,),
        device_id_type=MESH,
    )


class Exchange:
    def __init__(self, n, ref, sems):
        self.n, self.ref, self.sems = n, ref, sems
        self.me = lax.axis_index("dp")
        self.half = n // 2
        self.parity = lax.rem(self.me, 2)

    def own(self):
        return self.ref.at[self.me]

    def several(self, kind, count):
        blocks = self.ref.at[pl.ds(0, count)]
        return remote(blocks, blocks, self.sems, kind, mate())

    def relay(self):
        blocks = self.ref.reshape(self.half, 2, *self.ref.shape[1:]).at[:, self.parity]
        return remote(blocks, blocks, self.sems, self.last, mate())

    def forward(self):
        self.several(*self.counts[-1]).wait_recv()
        self.relay().start()

    def arrive(self):
        self.relay().wait_recv()

    def drain(self):
        for kind, count in self.counts:
            self.several(kind, count).wait_send()
        self.relay().wait_send()


class Share(Exchange):
    last = 1

    def __init__(self, n, ref, sems, own):
        super().__init__(n, ref, sems)
        self.counts = ((0, self.half),)
        self.source = own
        self.parity = 1 - lax.rem(self.me, 2)

    def start(self):
        def send(i):
            device = target(self.n, i)
            device = device + 1 - 2 * lax.rem(device, 2)
            remote(self.source, self.own(), self.sems, 0, device).start()

        each(0, self.half, send)


class Scatter(Exchange):
    def start(self):
        own = self.own()
        turn = 2 * (self.me // self.half) - 1

        def send(i):
            device = lax.rem(self.me + turn * i + self.n, self.n)
            remote(own, own, self.sems, 0, device).start()

        first = 1 + (self.n - 1) % 4
        for i in range(1, first):
            send(i)
        each(first, self.n, send, unroll=4)

    def arrive(self):
        self.several(0, self.n - 1).wait_recv()

    def drain(self):
        self.several(0, self.n - 1).wait_send()


class LineShare(Exchange):
    last = 2

    def __init__(self, n, ref, sems):
        super().__init__(n, ref, sems)
        self.lines = line_count(n)
        self.plane = n // self.lines
        self.peers = self.plane // 2
        self.spot = lax.rem(self.me, self.plane)
        self.counts = ((0, self.lines - 1), (1, self.lines * (self.peers - 1)))

    def across(self, j):
        block = self.ref.at[lax.rem(self.me - self.plane * j + self.n, self.n)]

        def send(k):
            device = self.me - self.spot + lax.rem(self.spot + 2 * k, self.plane)
            remote(block, block, self.sems, 1, device).start()

        each(1, self.peers, send)

    def start(self):
        own = self.own()
        for j in range(1, self.lines):
            remote(own, own, self.sems, 0, lax.rem(self.me + self.plane * j, self.n)).start()
        self.across(0)

    def spread(self):
        self.several(*self.counts[0]).wait_recv()
        for j in range(1, self.lines):
            self.across(j)


def line_count(n):
    return 4 if n % 8 == 0 else 1


def embed_kernel(
    n,
    x_hbm,
    gain_hbm,
    wq_hbm,
    wk_hbm,
    wv_hbm,
    wo_hbm,
    text_hbm,
    all_txt,
    abar0,
    abar1,
    abar2,
    emb_ref,
    text_ref,
    xs,
    gain_ref,
    wqks,
    wvs,
    wos,
    normed,
    qkn0,
    qkn1,
    pooled,
    zs,
    xbar,
    all_xbar,
    x_sem,
    q_sem,
    k_sem,
    w_sem,
    own0,
    own1,
    vs,
    share_sems,
):
    images, tokens, width = xs.shape
    groups = wqks.shape[0]
    cols = width // groups
    head = width // HEADS
    me = lax.axis_index("dp")
    abars = (abar0, abar1, abar2)

    def x_copy(i):
        return pltpu.make_async_copy(x_hbm.at[i], xs.at[i], x_sem.at[i])

    def q_copy(g):
        return pltpu.make_async_copy(
            wq_hbm.at[:, pl.ds(g * cols, cols)], wqks.at[g, :, pl.ds(0, cols)], q_sem.at[g]
        )

    def k_copy(g):
        return pltpu.make_async_copy(
            wk_hbm.at[:, pl.ds(g * cols, cols)], wqks.at[g, :, pl.ds(cols, cols)], k_sem.at[g]
        )

    v_copy = pltpu.make_async_copy(wv_hbm, wvs, w_sem.at[0])
    o_copy = pltpu.make_async_copy(wo_hbm, wos, w_sem.at[1])
    gain_copy = pltpu.make_async_copy(gain_hbm, gain_ref, w_sem.at[2])
    text_copy = pltpu.make_async_copy(text_hbm, text_ref, w_sem.at[3])
    gain_copy.start()
    for i in range(images):
        x_copy(i).start()
    text_copy.start()
    greet(n)
    for g in range(groups):
        q_copy(g).start()
        k_copy(g).start()
    v_copy.start()
    o_copy.start()

    txt_share = LineShare(n, all_txt, share_sems.at[0])
    xbar_share = LineShare(n, all_xbar, share_sems.at[1])

    pooled[...] = jnp.zeros_like(pooled)
    gain_copy.wait()
    gain = gain_ref[...]
    block = 32

    def norm_block(i, b, acc):
        x = xs[i, pl.ds(b * block, block), :].astype(F32)
        center = x - jnp.mean(x, axis=-1, keepdims=True)
        spread = jnp.mean(center * center, axis=-1, keepdims=True)
        out = center * lax.rsqrt(spread + epsilon) * gain
        rows = pl.ds(pl.multiple_of(i * tokens + b * block, block), block)
        normed[rows, :] = out.astype(BF16)
        return acc + jnp.sum(x, axis=0, keepdims=True)

    def mean_tokens(i, total):
        first = xs[i, pl.ds(0, 1), :].astype(F32)
        xbar[pl.ds(i, 1), :] = first + (total - first) / (tokens - 1)

    def norm_image(i, _):
        x_copy(i).wait()
        zero = jnp.zeros((1, width), F32)
        total = lax.fori_loop(
            0, tokens // block, lambda b, acc: norm_block(i, b, acc), zero, unroll=4
        )
        mean_tokens(i, total)
        return 0

    ahead = images // BLOCKS
    lax.fori_loop(0, ahead, norm_image, 0)
    seg_row = lax.broadcasted_iota(jnp.int32, (cols, cols), 0) // head
    seg_col = lax.broadcasted_iota(jnp.int32, (cols, cols), 1) // head
    seg = jnp.where(seg_row == seg_col, 1.0, 0.0).astype(BF16)
    lanes = 128
    per = lanes // head
    lane_head = lax.broadcasted_iota(jnp.int32, (tokens, lanes), 1) // head
    coef = jnp.where(
        lax.broadcasted_iota(jnp.int32, (tokens, 1), 0) == 0, 1.0, 1.0 / (tokens - 1)
    ).astype(F32)

    def unit(proj):
        sq = jnp.dot((proj * proj).astype(BF16), seg, preferred_element_type=F32)
        return (proj * lax.rsqrt(sq + epsilon)).astype(BF16)

    qkns = (qkn0, qkn1)

    def project(g, b):
        rows = pl.ds(b * (images * tokens // BLOCKS), images * tokens // BLOCKS)
        proj = jnp.dot(normed[rows, :], wqks[g], preferred_element_type=F32)
        qkn = qkns[g % 2]
        qkn[rows, 0:cols] = unit(proj[:, 0:cols])
        qkn[rows, cols : 2 * cols] = unit(proj[:, cols : 2 * cols])

    def attend(g, i):
        rows = pl.ds(i * tokens, tokens)
        qkn = qkns[g % 2]
        for pair in range(cols // lanes):
            lo = pair * lanes
            qi = qkn[rows, lo : lo + lanes]
            ki = qkn[rows, cols + lo : cols + lo + lanes]
            km = jnp.concatenate(
                [jnp.where(lane_head == h, ki, jnp.zeros_like(ki)) for h in range(per)],
                axis=0,
            )
            s = lax.dot_general(qi, km, NT, preferred_element_type=F32)
            e = jnp.exp2(s * (attn_temp * log2e))
            for h in range(per):
                eh = e[:, h * tokens : (h + 1) * tokens]
                scale = coef / jnp.sum(eh, axis=-1, keepdims=True)
                ph = jnp.sum(eh * scale, axis=0, keepdims=True)
                at = g * SLOTS + pair * per + h
                pooled[i, at : at + 1, :] = ph

    def weigh(low, high):
        rows = SLOTS * (high - low)
        wide = cols * (high - low)
        for i in range(images):
            p = pooled[i, low * SLOTS : high * SLOTS, :]
            hi = p.astype(BF16)
            lo = (p - hi.astype(F32)).astype(BF16)
            z2 = jnp.dot(
                jnp.concatenate([hi, lo], axis=0),
                normed[i * tokens : (i + 1) * tokens, :],
                preferred_element_type=F32,
            )
            z = z2[:rows] + z2[rows:]
            hi = z.astype(BF16)
            zs[0, i * rows : (i + 1) * rows, :] = hi
            zs[1, i * rows : (i + 1) * rows, :] = (z - hi.astype(F32)).astype(BF16)
        wv = wvs[:, low * cols : high * cols]
        full = jnp.dot(zs[0, : images * rows, :], wv, preferred_element_type=F32) + jnp.dot(
            zs[1, : images * rows, :], wv, preferred_element_type=F32
        )
        slot = lax.broadcasted_iota(jnp.int32, (rows, wide), 0)
        owner = lax.broadcasted_iota(jnp.int32, (rows, wide), 1) // head
        keep = slot == owner // GROUP * SLOTS + owner % GROUP
        picked = [
            jnp.sum(
                jnp.where(keep, full[i * rows : (i + 1) * rows, :], 0.0), axis=0, keepdims=True
            )
            for i in range(images)
        ]
        return jnp.concatenate(picked, axis=0).astype(BF16)

    def value(b):
        rows = pl.ds(b * (images * tokens // BLOCKS), images * tokens // BLOCKS)
        wv = wvs[:, width - cols : width]
        vs[rows, :] = jnp.dot(normed[rows, :], wv, preferred_element_type=F32).astype(BF16)

    def weigh_last():
        slot = lax.broadcasted_iota(jnp.int32, (2 * SLOTS, cols), 0)
        owner = lax.broadcasted_iota(jnp.int32, (2 * SLOTS, cols), 1) // head
        keep = lax.rem(slot, SLOTS) == owner
        picked = []
        for i in range(images):
            p = pooled[i, (groups - 1) * SLOTS : groups * SLOTS, :]
            hi = p.astype(BF16)
            lo = (p - hi.astype(F32)).astype(BF16)
            full = jnp.dot(
                jnp.concatenate([hi, lo], axis=0),
                vs[i * tokens : (i + 1) * tokens, :],
                preferred_element_type=F32,
            )
            picked.append(jnp.sum(jnp.where(keep, full, 0.0), axis=0, keepdims=True))
        return jnp.concatenate(picked, axis=0).astype(BF16)

    early, late, last = groups // 2, groups - 1, groups
    shares = [
        Share(n, abar0, share_sems.at[2], own0),
        Share(n, abar1, share_sems.at[3], own1),
        Scatter(n, abar2, share_sems.at[4]),
    ]
    for g in range(groups + 1):
        if g < groups:
            q_copy(g).wait()
            k_copy(g).wait()
        if g == 1:
            pl.semaphore_wait(pltpu.get_barrier_semaphore(), n - 1)
            xbar_share.start()
            txt_share.start()
        if g == early + 1:
            v_copy.wait()
            own0[...] = weigh(0, early)
            shares[0].start()
            xbar_share.spread()
        if g == groups:
            own1[...] = weigh(early, late)
            shares[1].start()
            txt_share.spread()
        if g == 0:
            for i in range(ahead, images):
                x_copy(i).wait()
            for i in range(ahead, images):
                total = jnp.zeros((1, width), F32)
                for b in range(tokens // block):
                    total = norm_block(i, b, total)
                mean_tokens(i, total)
            project(0, 0)
            for b in range(1, BLOCKS):
                project(0, b)
            all_xbar[me] = xbar[...].astype(BF16)
            text_copy.wait()
            text32 = text_ref[...].astype(F32)
            txt_norm = jnp.sqrt(jnp.sum(text32 * text32, axis=1, keepdims=True) + epsilon)
            all_txt[me] = (text32 / txt_norm).astype(BF16)
            continue
        for b in range(BLOCKS):
            if g == groups:
                value(b)
            if g > 0:
                for i in range(b * images // BLOCKS, (b + 1) * images // BLOCKS):
                    attend(g - 1, i)
            if g < groups:
                project(g, b)
    abars[2][me] = weigh_last()
    shares[2].start()
    xbar_share.forward()
    shares[0].forward()
    shares[1].forward()
    txt_share.forward()
    o_copy.wait()

    total = n * images
    chunk = min(total, 256)
    part = chunk // images

    def join(ref, r):
        return ref[r * part : (r + 1) * part].reshape(chunk, ref.shape[-1])

    def out_part(r, c, low, high):
        w = wos[low * cols : high * cols, :]
        return jnp.dot(join(abars[c], r), w, preferred_element_type=F32)

    for share in (xbar_share, *shares[:2]):
        share.arrive()
        share.drain()
    for r in range(total // chunk):
        emb = join(all_xbar, r).astype(F32) + out_part(r, 0, 0, early) + out_part(r, 1, early, late)
        emb_ref[r * chunk : (r + 1) * chunk, :] = emb
    shares[2].arrive()
    for r in range(total // chunk):
        emb_ref[r * chunk : (r + 1) * chunk, :] += out_part(r, 2, late, last)
    txt_share.arrive()
    for share in (txt_share, shares[2]):
        share.drain()


def embed(features, ln_gain, w_query, w_key, w_value, w_out, text_raw, n):
    images, tokens, width = features.shape
    groups = HEADS // GROUP
    cols = width // groups
    hbm = pl.BlockSpec(memory_space=pl.ANY)
    vmem = pl.BlockSpec(memory_space=pltpu.VMEM)
    args = (features, ln_gain.reshape(1, width), w_query, w_key, w_value, w_out, text_raw)
    args = [pltpu.with_memory_space_constraint(a, pltpu.HBM) for a in args]
    return pl.pallas_call(
        functools.partial(embed_kernel, n),
        out_shape=(
            pltpu.VMEM((n, images, width), BF16),
            pltpu.VMEM((n, images, width // 2), BF16),
            pltpu.VMEM((n, images, width // 4), BF16),
            pltpu.VMEM((n, images, width // 4), BF16),
            pltpu.VMEM((n * images, width), F32),
            pltpu.VMEM((images, width), BF16),
        ),
        in_specs=[hbm] * 7,
        out_specs=(vmem,) * 6,
        scratch_shapes=[
            pltpu.VMEM((images, tokens, width), BF16),
            pltpu.VMEM((1, width), F32),
            pltpu.VMEM((groups, width, 2 * cols), BF16),
            pltpu.VMEM((width, width), BF16),
            pltpu.VMEM((width, width), BF16),
            pltpu.VMEM((images * tokens, width), BF16),
            pltpu.VMEM((images * tokens, 2 * cols), BF16),
            pltpu.VMEM((images * tokens, 2 * cols), BF16),
            pltpu.VMEM((images, SLOTS * groups, tokens), F32),
            pltpu.VMEM((2, images * SLOTS * groups, width), BF16),
            pltpu.VMEM((images, width), F32),
            pltpu.VMEM((n, images, width), BF16),
            pltpu.SemaphoreType.DMA((images,)),
            pltpu.SemaphoreType.DMA((groups,)),
            pltpu.SemaphoreType.DMA((groups,)),
            pltpu.SemaphoreType.DMA((4,)),
            pltpu.VMEM((images, width // 2), BF16),
            pltpu.VMEM((images, width // 4), BF16),
            pltpu.VMEM((images * tokens, cols), BF16),
            pltpu.SemaphoreType.DMA((5, 6)),
        ],
        compiler_params=pltpu.CompilerParams(
            collective_id=0, has_side_effects=True, vmem_limit_bytes=40 * 2**20
        ),
        name="embed",
    )(*args)


def loss_kernel(
    txt_ref,
    abar0,
    abar1,
    abar2,
    emb_ref,
    text_ref,
    loss_hbm,
    text_grad_hbm,
    w_hbm,
    img_s,
    grad_s,
    w_s,
    loss_s,
    text_grad_s,
    out_sem,
):
    total, width = emb_ref.shape
    images = text_ref.shape[0]
    chunk = min(total, 256)
    chunks = [slice(r, r + chunk) for r in range(0, total, chunk)]
    pieces = 4
    rows = width // pieces

    def w_copy(c):
        return pltpu.make_async_copy(
            w_s.at[pl.ds(c * rows, rows), :], w_hbm.at[pl.ds(c * rows, rows), :], out_sem.at[c]
        )

    loss_copy = pltpu.make_async_copy(loss_s, loss_hbm, out_sem.at[pieces])
    text_copy = pltpu.make_async_copy(text_grad_s, text_grad_hbm, out_sem.at[pieces + 1])

    def eye(r):
        row = lax.broadcasted_iota(jnp.int32, (chunk, total), 0) + r.start
        return row == lax.broadcasted_iota(jnp.int32, (chunk, total), 1)

    def abar(low, wide):
        for ref in (abar0, abar1, abar2):
            if low < ref.shape[1]:
                return ref[:, low : low + wide]
            low -= ref.shape[1]

    txt = txt_ref[...]
    invs, es, rowsums = [], [], []
    colsum = rowsum_flat = jnp.zeros((1, total), F32)
    diag = jnp.zeros((1, total), F32)
    for r in chunks:
        emb = emb_ref[r, :]
        inv = lax.rsqrt(jnp.sum(emb * emb, axis=1, keepdims=True) + epsilon)
        img = (emb * inv).astype(BF16)
        img_s[r, :] = img
        logits = inv_temp * lax.dot_general(img, txt, NT, preferred_element_type=F32)
        e = jnp.exp(logits)
        rowsum = jnp.sum(e, axis=1, keepdims=True)
        colsum = colsum + jnp.sum(e, axis=0, keepdims=True)
        rowsum_flat = rowsum_flat + jnp.sum(jnp.where(eye(r), rowsum, 0.0), axis=0, keepdims=True)
        diag = diag + jnp.sum(jnp.where(eye(r), logits, 0.0), axis=0, keepdims=True)
        invs.append(inv)
        es.append(e)
        rowsums.append(rowsum)

    half_col = 0.5 / colsum
    text32 = text_ref[...].astype(F32)
    txt_norm = jnp.sqrt(jnp.sum(text32 * text32, axis=1, keepdims=True) + epsilon)
    txt_f = text32 / txt_norm
    img = img_s[...]
    own = inv_temp * lax.dot_general(txt_f.astype(BF16), img, NT, preferred_element_type=F32)

    for r, inv, e, rowsum in zip(chunks, invs, es, rowsums):
        delta = e * (0.5 / rowsum + half_col) - jnp.where(eye(r), 1.0, 0.0)
        grad = jnp.dot(delta.astype(BF16), txt, preferred_element_type=F32)
        emb = emb_ref[r, :]
        along = jnp.sum(emb * grad, axis=1, keepdims=True) * (inv * inv)
        grad_s[r, :] = ((grad - emb * along) * (inv_temp * inv)).astype(BF16)

    loss = jnp.sum(jnp.log(rowsum_flat) + jnp.log(colsum) - 2.0 * diag, axis=1, keepdims=True)
    loss_s[...] = loss / (2.0 * total)
    own_e = jnp.exp(own)
    own_sum = jnp.sum(own_e, axis=1, keepdims=True)
    col = lax.broadcasted_iota(jnp.int32, (images, total), 1)
    row = lax.broadcasted_iota(jnp.int32, (images, total), 0) + lax.axis_index("dp") * images
    own_delta = 0.5 * (own_e / rowsum_flat + own_e / own_sum) - jnp.where(col == row, 1.0, 0.0)
    grad_txt = inv_temp * jnp.dot(own_delta.astype(BF16), img, preferred_element_type=F32)
    text_grad_s[...] = (
        grad_txt - txt_f * jnp.sum(txt_f * grad_txt, axis=1, keepdims=True)
    ) / txt_norm

    for c in range(pieces):
        w_s[c * rows : (c + 1) * rows, :] = lax.dot_general(
            abar(c * rows, rows), grad_s[...], TN, preferred_element_type=F32
        ).astype(BF16)
        w_copy(c).start()
        if c == 0:
            loss_copy.start()
            text_copy.start()
    for c in range(pieces):
        w_copy(c).wait()
    loss_copy.wait()
    text_copy.wait()


def finish(all_txt, abars, emb, text_raw):
    images, width = text_raw.shape
    total = emb.shape[0]
    vmem = pl.BlockSpec(memory_space=pltpu.VMEM)
    hbm = pl.BlockSpec(memory_space=pl.ANY)
    loss, text_grad, w_grad = pl.pallas_call(
        loss_kernel,
        out_shape=(
            jax.ShapeDtypeStruct((1, 1), F32),
            jax.ShapeDtypeStruct((images, width), F32),
            jax.ShapeDtypeStruct((width, width), BF16),
        ),
        in_specs=[vmem] * 6,
        out_specs=(hbm,) * 3,
        scratch_shapes=[
            pltpu.VMEM((total, width), BF16),
            pltpu.VMEM((total, width), BF16),
            pltpu.VMEM((width, width), BF16),
            pltpu.VMEM((1, 1), F32),
            pltpu.VMEM((images, width), F32),
            pltpu.SemaphoreType.DMA((6,)),
        ],
        compiler_params=pltpu.CompilerParams(vmem_limit_bytes=40 * 2**20),
        name="finish",
    )(all_txt, *abars, emb, text_raw)
    return loss.reshape(()), text_grad, w_grad


def solution(mesh):
    n = mesh.shape["dp"]

    def local(features, ln_gain, w_query, w_key, w_value, w_out, text_raw):
        all_txt, *abars, emb, text = embed(
            features, ln_gain, w_query, w_key, w_value, w_out, text_raw, n
        )
        pairs = n * text_raw.shape[0]
        abars = [a.reshape(pairs, -1) for a in abars]
        return finish(all_txt.reshape(pairs, -1), abars, emb, text)

    placed = (P("dp", None, None), P(), P(), P(), P(), P(), P("dp", None))
    return jax.shard_map(
        local, mesh=mesh, in_specs=placed, out_specs=(P(), P("dp", None), P()), check_vma=False
    )
```

```python
import functools

import jax
import jax.numpy as jnp
from jax import lax
from jax.experimental import pallas as pl
from jax.experimental.pallas import tpu as pltpu
from jax.sharding import PartitionSpec as P

HEADS = 16
GROUP = 4
BLOCKS = 2
SLOTS = 8

inv_temp = 1.0 / 0.07
attn_temp = 8.0
epsilon = 1e-06
log2e = 1.4426950408889634

F32 = jnp.float32
BF16 = jnp.bfloat16
NT = (((1,), (1,)), ((), ()))
TN = (((0,), (0,)), ((), ()))


MESH = pl.DeviceIdType.MESH


def target(n, i):
    return lax.rem(lax.axis_index("dp") + 2 * i, n)


def mate():
    me = lax.axis_index("dp")
    return me + 1 - 2 * lax.rem(me, 2)


def greet(n):
    barrier = pltpu.get_barrier_semaphore()
    me = lax.axis_index("dp")

    def hello(i, _):
        pl.semaphore_signal(
            barrier, inc=1, device_id=(lax.rem(me + i, n),), device_id_type=MESH
        )
        return 0

    lax.fori_loop(1, n, hello, 0)


def each(low, high, act, unroll=1):
    def step(i, _):
        act(i)
        return 0

    lax.fori_loop(low, high, step, 0, unroll=unroll)


def remote(src, dst, sems, kind, device):
    return pltpu.make_async_remote_copy(
        src_ref=src,
        dst_ref=dst,
        send_sem=sems.at[2 * kind],
        recv_sem=sems.at[2 * kind + 1],
        device_id=(device,),
        device_id_type=MESH,
    )


class Exchange:
    def __init__(self, n, ref, sems):
        self.n, self.ref, self.sems = n, ref, sems
        self.me = lax.axis_index("dp")
        self.half = n // 2
        self.parity = lax.rem(self.me, 2)

    def own(self):
        return self.ref.at[self.me]

    def several(self, kind, count):
        blocks = self.ref.at[pl.ds(0, count)]
        return remote(blocks, blocks, self.sems, kind, mate())

    def relay(self):
        blocks = self.ref.reshape(self.half, 2, *self.ref.shape[1:]).at[:, self.parity]
        return remote(blocks, blocks, self.sems, self.last, mate())

    def forward(self):
        self.several(*self.counts[-1]).wait_recv()
        self.relay().start()

    def arrive(self):
        self.relay().wait_recv()

    def drain(self):
        for kind, count in self.counts:
            self.several(kind, count).wait_send()
        self.relay().wait_send()


class Share(Exchange):
    last = 1

    def __init__(self, n, ref, sems, own):
        super().__init__(n, ref, sems)
        self.counts = ((0, self.half),)
        self.source = own
        self.parity = 1 - lax.rem(self.me, 2)

    def start(self):
        def send(i):
            device = target(self.n, i)
            device = device + 1 - 2 * lax.rem(device, 2)
            remote(self.source, self.own(), self.sems, 0, device).start()

        each(0, self.half, send)


class Scatter(Exchange):
    def start(self):
        own = self.own()
        turn = 2 * (self.me // self.half) - 1

        def send(i):
            device = lax.rem(self.me + turn * i + self.n, self.n)
            remote(own, own, self.sems, 0, device).start()

        first = 1 + (self.n - 1) % 4
        for i in range(1, first):
            send(i)
        each(first, self.n, send, unroll=4)

    def arrive(self):
        self.several(0, self.n - 1).wait_recv()

    def drain(self):
        self.several(0, self.n - 1).wait_send()


class LineShare(Exchange):
    last = 2

    def __init__(self, n, ref, sems):
        super().__init__(n, ref, sems)
        self.lines = line_count(n)
        self.plane = n // self.lines
        self.peers = self.plane // 2
        self.spot = lax.rem(self.me, self.plane)
        self.counts = ((0, self.lines - 1), (1, self.lines * (self.peers - 1)))

    def across(self, j):
        block = self.ref.at[lax.rem(self.me - self.plane * j + self.n, self.n)]

        def send(k):
            device = self.me - self.spot + lax.rem(self.spot + 2 * k, self.plane)
            remote(block, block, self.sems, 1, device).start()

        each(1, self.peers, send)

    def start(self):
        own = self.own()
        for j in range(1, self.lines):
            remote(own, own, self.sems, 0, lax.rem(self.me + self.plane * j, self.n)).start()
        self.across(0)

    def spread(self):
        self.several(*self.counts[0]).wait_recv()
        for j in range(1, self.lines):
            self.across(j)


def line_count(n):
    return 4 if n % 8 == 0 else 1


def embed_kernel(
    n,
    x_hbm,
    gain_hbm,
    wq_hbm,
    wk_hbm,
    wv_hbm,
    wo_hbm,
    text_hbm,
    all_txt,
    abar0,
    abar1,
    abar2,
    emb_ref,
    text_ref,
    xs,
    gain_ref,
    wqks,
    wvs,
    wos,
    normed,
    qkn0,
    qkn1,
    pooled,
    zs,
    xbar,
    all_xbar,
    x_sem,
    q_sem,
    k_sem,
    w_sem,
    own0,
    own1,
    vs,
    xbar_sems,
    txt_sems,
    sems0,
    sems1,
    sems2,
):
    images, tokens, width = xs.shape
    groups = wqks.shape[0]
    cols = width // groups
    head = width // HEADS
    me = lax.axis_index("dp")
    abars = (abar0, abar1, abar2)

    def x_copy(i):
        return pltpu.make_async_copy(x_hbm.at[i], xs.at[i], x_sem.at[i])

    def q_copy(g):
        return pltpu.make_async_copy(
            wq_hbm.at[:, pl.ds(g * cols, cols)], wqks.at[g, :, pl.ds(0, cols)], q_sem.at[g]
        )

    def k_copy(g):
        return pltpu.make_async_copy(
            wk_hbm.at[:, pl.ds(g * cols, cols)], wqks.at[g, :, pl.ds(cols, cols)], k_sem.at[g]
        )

    v_copy = pltpu.make_async_copy(wv_hbm, wvs, w_sem.at[0])
    o_copy = pltpu.make_async_copy(wo_hbm, wos, w_sem.at[1])
    gain_copy = pltpu.make_async_copy(gain_hbm, gain_ref, w_sem.at[2])
    text_copy = pltpu.make_async_copy(text_hbm, text_ref, w_sem.at[3])
    gain_copy.start()
    for i in range(images):
        x_copy(i).start()
    text_copy.start()
    greet(n)
    for g in range(groups):
        q_copy(g).start()
        k_copy(g).start()
    v_copy.start()
    o_copy.start()

    txt_share = LineShare(n, all_txt, txt_sems)
    xbar_share = LineShare(n, all_xbar, xbar_sems)

    pooled[...] = jnp.zeros_like(pooled)
    gain_copy.wait()
    gain = gain_ref[...]
    block = 32

    def norm_block(i, b, acc):
        x = xs[i, pl.ds(b * block, block), :].astype(F32)
        center = x - jnp.mean(x, axis=-1, keepdims=True)
        spread = jnp.mean(center * center, axis=-1, keepdims=True)
        out = center * lax.rsqrt(spread + epsilon) * gain
        rows = pl.ds(pl.multiple_of(i * tokens + b * block, block), block)
        normed[rows, :] = out.astype(BF16)
        return acc + jnp.sum(x, axis=0, keepdims=True)

    def mean_tokens(i, total):
        first = xs[i, pl.ds(0, 1), :].astype(F32)
        xbar[pl.ds(i, 1), :] = first + (total - first) / (tokens - 1)

    def norm_image(i, _):
        x_copy(i).wait()
        zero = jnp.zeros((1, width), F32)
        total = lax.fori_loop(
            0, tokens // block, lambda b, acc: norm_block(i, b, acc), zero, unroll=4
        )
        mean_tokens(i, total)
        return 0

    ahead = images // BLOCKS
    lax.fori_loop(0, ahead, norm_image, 0)
    seg_row = lax.broadcasted_iota(jnp.int32, (cols, cols), 0) // head
    seg_col = lax.broadcasted_iota(jnp.int32, (cols, cols), 1) // head
    seg = jnp.where(seg_row == seg_col, 1.0, 0.0).astype(BF16)
    lanes = 128
    per = lanes // head
    lane_head = lax.broadcasted_iota(jnp.int32, (tokens, lanes), 1) // head
    coef = jnp.where(
        lax.broadcasted_iota(jnp.int32, (tokens, 1), 0) == 0, 1.0, 1.0 / (tokens - 1)
    ).astype(F32)

    def unit(proj):
        sq = jnp.dot((proj * proj).astype(BF16), seg, preferred_element_type=F32)
        return (proj * lax.rsqrt(sq + epsilon)).astype(BF16)

    qkns = (qkn0, qkn1)

    def project(g, b):
        rows = pl.ds(b * (images * tokens // BLOCKS), images * tokens // BLOCKS)
        proj = jnp.dot(normed[rows, :], wqks[g], preferred_element_type=F32)
        qkn = qkns[g % 2]
        qkn[rows, 0:cols] = unit(proj[:, 0:cols])
        qkn[rows, cols : 2 * cols] = unit(proj[:, cols : 2 * cols])

    def attend(g, i):
        rows = pl.ds(i * tokens, tokens)
        qkn = qkns[g % 2]
        for pair in range(cols // lanes):
            lo = pair * lanes
            qi = qkn[rows, lo : lo + lanes]
            ki = qkn[rows, cols + lo : cols + lo + lanes]
            km = jnp.concatenate(
                [jnp.where(lane_head == h, ki, jnp.zeros_like(ki)) for h in range(per)],
                axis=0,
            )
            s = lax.dot_general(qi, km, NT, preferred_element_type=F32)
            e = jnp.exp2(s * (attn_temp * log2e))
            for h in range(per):
                eh = e[:, h * tokens : (h + 1) * tokens]
                scale = coef / jnp.sum(eh, axis=-1, keepdims=True)
                ph = jnp.sum(eh * scale, axis=0, keepdims=True)
                at = g * SLOTS + pair * per + h
                pooled[i, at : at + 1, :] = ph

    def weigh(low, high):
        rows = SLOTS * (high - low)
        wide = cols * (high - low)
        for i in range(images):
            p = pooled[i, low * SLOTS : high * SLOTS, :]
            hi = p.astype(BF16)
            lo = (p - hi.astype(F32)).astype(BF16)
            z2 = jnp.dot(
                jnp.concatenate([hi, lo], axis=0),
                normed[i * tokens : (i + 1) * tokens, :],
                preferred_element_type=F32,
            )
            z = z2[:rows] + z2[rows:]
            hi = z.astype(BF16)
            zs[0, i * rows : (i + 1) * rows, :] = hi
            zs[1, i * rows : (i + 1) * rows, :] = (z - hi.astype(F32)).astype(BF16)
        wv = wvs[:, low * cols : high * cols]
        full = jnp.dot(zs[0, : images * rows, :], wv, preferred_element_type=F32) + jnp.dot(
            zs[1, : images * rows, :], wv, preferred_element_type=F32
        )
        slot = lax.broadcasted_iota(jnp.int32, (rows, wide), 0)
        owner = lax.broadcasted_iota(jnp.int32, (rows, wide), 1) // head
        keep = slot == owner // GROUP * SLOTS + owner % GROUP
        picked = [
            jnp.sum(
                jnp.where(keep, full[i * rows : (i + 1) * rows, :], 0.0), axis=0, keepdims=True
            )
            for i in range(images)
        ]
        return jnp.concatenate(picked, axis=0).astype(BF16)

    def value(b):
        rows = pl.ds(b * (images * tokens // BLOCKS), images * tokens // BLOCKS)
        wv = wvs[:, width - cols : width]
        vs[rows, :] = jnp.dot(normed[rows, :], wv, preferred_element_type=F32).astype(BF16)

    def weigh_last():
        slot = lax.broadcasted_iota(jnp.int32, (2 * SLOTS, cols), 0)
        owner = lax.broadcasted_iota(jnp.int32, (2 * SLOTS, cols), 1) // head
        keep = lax.rem(slot, SLOTS) == owner
        picked = []
        for i in range(images):
            p = pooled[i, (groups - 1) * SLOTS : groups * SLOTS, :]
            hi = p.astype(BF16)
            lo = (p - hi.astype(F32)).astype(BF16)
            full = jnp.dot(
                jnp.concatenate([hi, lo], axis=0),
                vs[i * tokens : (i + 1) * tokens, :],
                preferred_element_type=F32,
            )
            picked.append(jnp.sum(jnp.where(keep, full, 0.0), axis=0, keepdims=True))
        return jnp.concatenate(picked, axis=0).astype(BF16)

    early, late, last = groups // 2, groups - 1, groups
    shares = [
        Share(n, abar0, sems0, own0),
        Share(n, abar1, sems1, own1),
        Scatter(n, abar2, sems2),
    ]
    for g in range(groups + 1):
        if g < groups:
            q_copy(g).wait()
            k_copy(g).wait()
        if g == 1:
            pl.semaphore_wait(pltpu.get_barrier_semaphore(), n - 1)
            xbar_share.start()
            txt_share.start()
        if g == early + 1:
            v_copy.wait()
            own0[...] = weigh(0, early)
            shares[0].start()
            xbar_share.spread()
        if g == groups:
            own1[...] = weigh(early, late)
            shares[1].start()
            txt_share.spread()
        if g == 0:
            for i in range(ahead, images):
                x_copy(i).wait()
            for i in range(ahead, images):
                total = jnp.zeros((1, width), F32)
                for b in range(tokens // block):
                    total = norm_block(i, b, total)
                mean_tokens(i, total)
            project(0, 0)
            for b in range(1, BLOCKS):
                project(0, b)
            all_xbar[me] = xbar[...].astype(BF16)
            text_copy.wait()
            text32 = text_ref[...].astype(F32)
            txt_norm = jnp.sqrt(jnp.sum(text32 * text32, axis=1, keepdims=True) + epsilon)
            all_txt[me] = (text32 / txt_norm).astype(BF16)
            continue
        for b in range(BLOCKS):
            if g == groups:
                value(b)
            if g > 0:
                for i in range(b * images // BLOCKS, (b + 1) * images // BLOCKS):
                    attend(g - 1, i)
            if g < groups:
                project(g, b)
    abars[2][me] = weigh_last()
    shares[2].start()
    xbar_share.forward()
    shares[0].forward()
    shares[1].forward()
    txt_share.forward()
    o_copy.wait()

    total = n * images
    chunk = min(total, 256)
    part = chunk // images

    def join(ref, r):
        return ref[r * part : (r + 1) * part].reshape(chunk, ref.shape[-1])

    def out_part(r, c, low, high):
        w = wos[low * cols : high * cols, :]
        return jnp.dot(join(abars[c], r), w, preferred_element_type=F32)

    for share in (xbar_share, *shares[:2]):
        share.arrive()
        share.drain()
    for r in range(total // chunk):
        emb = join(all_xbar, r).astype(F32) + out_part(r, 0, 0, early) + out_part(r, 1, early, late)
        emb_ref[r * chunk : (r + 1) * chunk, :] = emb
    shares[2].arrive()
    for r in range(total // chunk):
        emb_ref[r * chunk : (r + 1) * chunk, :] += out_part(r, 2, late, last)
    txt_share.arrive()
    for share in (txt_share, shares[2]):
        share.drain()


def embed(features, ln_gain, w_query, w_key, w_value, w_out, text_raw, n):
    images, tokens, width = features.shape
    groups = HEADS // GROUP
    cols = width // groups
    hbm = pl.BlockSpec(memory_space=pl.ANY)
    vmem = pl.BlockSpec(memory_space=pltpu.VMEM)
    args = (features, ln_gain.reshape(1, width), w_query, w_key, w_value, w_out, text_raw)
    args = [pltpu.with_memory_space_constraint(a, pltpu.HBM) for a in args]
    return pl.pallas_call(
        functools.partial(embed_kernel, n),
        out_shape=(
            pltpu.VMEM((n, images, width), BF16),
            pltpu.VMEM((n, images, width // 2), BF16),
            pltpu.VMEM((n, images, width // 4), BF16),
            pltpu.VMEM((n, images, width // 4), BF16),
            pltpu.VMEM((n * images, width), F32),
            pltpu.VMEM((images, width), BF16),
        ),
        in_specs=[hbm] * 7,
        out_specs=(vmem,) * 6,
        scratch_shapes=[
            pltpu.VMEM((images, tokens, width), BF16),
            pltpu.VMEM((1, width), F32),
            pltpu.VMEM((groups, width, 2 * cols), BF16),
            pltpu.VMEM((width, width), BF16),
            pltpu.VMEM((width, width), BF16),
            pltpu.VMEM((images * tokens, width), BF16),
            pltpu.VMEM((images * tokens, 2 * cols), BF16),
            pltpu.VMEM((images * tokens, 2 * cols), BF16),
            pltpu.VMEM((images, SLOTS * groups, tokens), F32),
            pltpu.VMEM((2, images * SLOTS * groups, width), BF16),
            pltpu.VMEM((images, width), F32),
            pltpu.VMEM((n, images, width), BF16),
            pltpu.SemaphoreType.DMA((images,)),
            pltpu.SemaphoreType.DMA((groups,)),
            pltpu.SemaphoreType.DMA((groups,)),
            pltpu.SemaphoreType.DMA((4,)),
            pltpu.VMEM((images, width // 2), BF16),
            pltpu.VMEM((images, width // 4), BF16),
            pltpu.VMEM((images * tokens, cols), BF16),
            pltpu.SemaphoreType.DMA((6,)),
            pltpu.SemaphoreType.DMA((6,)),
            pltpu.SemaphoreType.DMA((4,)),
            pltpu.SemaphoreType.DMA((4,)),
            pltpu.SemaphoreType.DMA((2,)),
        ],
        compiler_params=pltpu.CompilerParams(
            collective_id=0, has_side_effects=True, vmem_limit_bytes=40 * 2**20
        ),
        name="embed",
    )(*args)


def loss_kernel(
    txt_ref,
    abar0,
    abar1,
    abar2,
    emb_ref,
    text_ref,
    loss_hbm,
    text_grad_hbm,
    w_hbm,
    img_s,
    grad_s,
    w_s,
    loss_s,
    text_grad_s,
    out_sem,
):
    total, width = emb_ref.shape
    images = text_ref.shape[0]
    chunk = min(total, 256)
    chunks = [slice(r, r + chunk) for r in range(0, total, chunk)]
    pieces = 4
    rows = width // pieces

    def w_copy(c):
        return pltpu.make_async_copy(
            w_s.at[pl.ds(c * rows, rows), :], w_hbm.at[pl.ds(c * rows, rows), :], out_sem.at[c]
        )

    loss_copy = pltpu.make_async_copy(loss_s, loss_hbm, out_sem.at[pieces])
    text_copy = pltpu.make_async_copy(text_grad_s, text_grad_hbm, out_sem.at[pieces + 1])

    def eye(r):
        row = lax.broadcasted_iota(jnp.int32, (chunk, total), 0) + r.start
        return row == lax.broadcasted_iota(jnp.int32, (chunk, total), 1)

    def abar(low, wide):
        for ref in (abar0, abar1, abar2):
            if low < ref.shape[1]:
                return ref[:, low : low + wide]
            low -= ref.shape[1]

    txt = txt_ref[...]
    invs, es, rowsums = [], [], []
    colsum = rowsum_flat = jnp.zeros((1, total), F32)
    diag = jnp.zeros((1, total), F32)
    for r in chunks:
        emb = emb_ref[r, :]
        inv = lax.rsqrt(jnp.sum(emb * emb, axis=1, keepdims=True) + epsilon)
        img = (emb * inv).astype(BF16)
        img_s[r, :] = img
        logits = inv_temp * lax.dot_general(img, txt, NT, preferred_element_type=F32)
        e = jnp.exp(logits)
        rowsum = jnp.sum(e, axis=1, keepdims=True)
        colsum = colsum + jnp.sum(e, axis=0, keepdims=True)
        rowsum_flat = rowsum_flat + jnp.sum(jnp.where(eye(r), rowsum, 0.0), axis=0, keepdims=True)
        diag = diag + jnp.sum(jnp.where(eye(r), logits, 0.0), axis=0, keepdims=True)
        invs.append(inv)
        es.append(e)
        rowsums.append(rowsum)

    half_col = 0.5 / colsum
    text32 = text_ref[...].astype(F32)
    txt_norm = jnp.sqrt(jnp.sum(text32 * text32, axis=1, keepdims=True) + epsilon)
    txt_f = text32 / txt_norm
    img = img_s[...]
    own = inv_temp * lax.dot_general(txt_f.astype(BF16), img, NT, preferred_element_type=F32)

    for r, inv, e, rowsum in zip(chunks, invs, es, rowsums):
        delta = e * (0.5 / rowsum + half_col) - jnp.where(eye(r), 1.0, 0.0)
        grad = jnp.dot(delta.astype(BF16), txt, preferred_element_type=F32)
        emb = emb_ref[r, :]
        along = jnp.sum(emb * grad, axis=1, keepdims=True) * (inv * inv)
        grad_s[r, :] = ((grad - emb * along) * (inv_temp * inv)).astype(BF16)

    loss = jnp.sum(jnp.log(rowsum_flat) + jnp.log(colsum) - 2.0 * diag, axis=1, keepdims=True)
    loss_s[...] = loss / (2.0 * total)
    own_e = jnp.exp(own)
    own_sum = jnp.sum(own_e, axis=1, keepdims=True)
    col = lax.broadcasted_iota(jnp.int32, (images, total), 1)
    row = lax.broadcasted_iota(jnp.int32, (images, total), 0) + lax.axis_index("dp") * images
    own_delta = 0.5 * (own_e / rowsum_flat + own_e / own_sum) - jnp.where(col == row, 1.0, 0.0)
    grad_txt = inv_temp * jnp.dot(own_delta.astype(BF16), img, preferred_element_type=F32)
    text_grad_s[...] = (
        grad_txt - txt_f * jnp.sum(txt_f * grad_txt, axis=1, keepdims=True)
    ) / txt_norm

    for c in range(pieces):
        w_s[c * rows : (c + 1) * rows, :] = lax.dot_general(
            abar(c * rows, rows), grad_s[...], TN, preferred_element_type=F32
        ).astype(BF16)
        w_copy(c).start()
        if c == 0:
            loss_copy.start()
            text_copy.start()
    for c in range(pieces):
        w_copy(c).wait()
    loss_copy.wait()
    text_copy.wait()


def finish(all_txt, abars, emb, text_raw):
    images, width = text_raw.shape
    total = emb.shape[0]
    vmem = pl.BlockSpec(memory_space=pltpu.VMEM)
    hbm = pl.BlockSpec(memory_space=pl.ANY)
    loss, text_grad, w_grad = pl.pallas_call(
        loss_kernel,
        out_shape=(
            jax.ShapeDtypeStruct((1, 1), F32),
            jax.ShapeDtypeStruct((images, width), F32),
            jax.ShapeDtypeStruct((width, width), BF16),
        ),
        in_specs=[vmem] * 6,
        out_specs=(hbm,) * 3,
        scratch_shapes=[
            pltpu.VMEM((total, width), BF16),
            pltpu.VMEM((total, width), BF16),
            pltpu.VMEM((width, width), BF16),
            pltpu.VMEM((1, 1), F32),
            pltpu.VMEM((images, width), F32),
            pltpu.SemaphoreType.DMA((6,)),
        ],
        compiler_params=pltpu.CompilerParams(vmem_limit_bytes=40 * 2**20),
        name="finish",
    )(all_txt, *abars, emb, text_raw)
    return loss.reshape(()), text_grad, w_grad


def solution(mesh):
    n = mesh.shape["dp"]

    def local(features, ln_gain, w_query, w_key, w_value, w_out, text_raw):
        all_txt, *abars, emb, text = embed(
            features, ln_gain, w_query, w_key, w_value, w_out, text_raw, n
        )
        pairs = n * text_raw.shape[0]
        abars = [a.reshape(pairs, -1) for a in abars]
        return finish(all_txt.reshape(pairs, -1), abars, emb, text)

    placed = (P("dp", None, None), P(), P(), P(), P(), P(), P("dp", None))
    return jax.shard_map(
        local, mesh=mesh, in_specs=placed, out_specs=(P(), P("dp", None), P()), check_vma=False
    )
```
